32 devices in a mesh: gx: 8 (over z, y), gy: 4 (over x, core).
Axes of the slice: x: 2, y: 2, z: 4, core: 2. Of those that a mesh axis runs over, the one named last changes fastest.
Arguments:
- preserved_vector: float32 [14, 64, 32, 128], P(None, 'gx', 'gy'), may hold values from -200 to 200, as said below
- nasa_table: float32 [32, 6], replicated, may hold values from -4 to 4.5, as said below
- gas_constant: float32 [32], replicated, may hold values from 0.3 to 3
- species_index: int32 [9], replicated, may hold values from 0 to 31, as said below
- face_kind: int32 [8, 4, 2], P('gx', 'gy'), may hold values from 0 to 1
Outputs:
- increment: float32 [14, 64, 32, 128], P(None, 'gx', 'gy')
The draws below stay inside these ranges and needn't reach their ends.
Inputs may be any that keep to these rules, and one draw needn't show every extreme that they name: `preserved_vector`: every cell is a physical state: positive partial densities and an energy whose temperature lies between 0.5 and 2.5. `nasa_table`: each row's cp over R polynomial exceeds 1.5 for temperatures 0.3 to 3. `species_index`: 9 distinct rows.
All inputs are finite; a program needn't handle non-finite values.
Results may differ from the reference program's by a relative error of at most 0.0003.
Values sent between devices are 32-bit elements; how exact they have to be, the bound alone decides.
A program may use at most 64 MiB of HBM per device.

```python
import math
import jax
import jax.numpy as jnp
from jax import lax

NS = 9
NVAR = 14
KINDS = 32
NEWTON = 2
CX = 8
CY = 8
NX = 64
NY = 32
NZ = 128
N_GX = 8
N_GY = 4


def thermo_tables(key):
    lower = jnp.array([2.5, 0.0, -0.05, -0.01, -0.002, -4.0], jnp.float32)
    upper = jnp.array([4.5, 0.6, 0.05, 0.01, 0.002, 4.0], jnp.float32)
    table = lower + (upper - lower) * jax.random.uniform(jax.random.fold_in(key, 101), (KINDS, 6), jnp.float32)
    gases = jnp.exp(jax.random.uniform(jax.random.fold_in(key, 102), (KINDS,), jnp.float32, math.log(0.3), math.log(3.0)))
    middle_rows = (jax.random.permutation(jax.random.fold_in(key, 103), KINDS - 2)[:NS - 2] + 1).astype(jnp.int32)
    end_rows = jnp.array([0, KINDS - 1], jnp.int32)
    pooled = jnp.concatenate([end_rows, middle_rows], axis=0)
    shuffle = jax.random.permutation(jax.random.fold_in(key, 104), NS).astype(jnp.int32)
    chosen = pooled[shuffle].astype(jnp.int32)
    return (table, gases, chosen)


def draw_nasa_table(key, part):
    return thermo_tables(key)[0]


def draw_gas_constant(key, part):
    return thermo_tables(key)[1]


def draw_species_index(key, part):
    return thermo_tables(key)[2]


def draw_preserved_vector(key, part):
    table, gases, chosen = thermo_tables(key)
    nasa_table_weights = table[chosen]
    component_kind_r_factor = gases[chosen]
    grid_sizes_list = (NX, NY, NZ)
    draw_seed_handles_list = [jax.random.fold_in(key, 200 + number) for number in range(6)]
    abscissa_place = (jnp.arange(NX, dtype=jnp.float32) / NX)[:, None, None]
    ordinate_place = (jnp.arange(NY, dtype=jnp.float32) / NY)[None, :, None]
    ramp = 0.3 + 1.35 * (abscissa_place + ordinate_place)
    bulk_compactness = jnp.exp(jax.random.uniform(draw_seed_handles_list[0], grid_sizes_list, jnp.float32, -0.4, 0.4))
    fractions = jax.nn.softmax(jax.random.normal(draw_seed_handles_list[1], (NS,) + grid_sizes_list, jnp.float32), axis=0)
    passive = jax.random.uniform(draw_seed_handles_list[2], grid_sizes_list, jnp.float32)
    kelvin_reading = jax.random.uniform(draw_seed_handles_list[3], grid_sizes_list, jnp.float32, 0.5, 2.4)
    velocity = 0.5 * ramp[None] * jnp.clip(jax.random.normal(draw_seed_handles_list[4], (3,) + grid_sizes_list, jnp.float32), -4.0, 4.0)
    prefix_addition_result = bulk_compactness[None] * fractions
    replicated_layer = kelvin_reading[None]
    columns = [nasa_table_weights[:, degree].reshape((NS, 1, 1, 1)) for degree in range(6)]
    chemical_heat_content = columns[5] + replicated_layer * (columns[0] + replicated_layer * (columns[1] / 2.0 + replicated_layer * (columns[2] / 3.0 + replicated_layer * (columns[3] / 4.0 + replicated_layer * columns[4] / 5.0))))
    caloric_tiers = component_kind_r_factor.reshape((NS, 1, 1, 1)) * (chemical_heat_content - replicated_layer)
    energy = jnp.sum(prefix_addition_result * caloric_tiers, axis=0) + 0.5 * bulk_compactness * jnp.sum(velocity * velocity, axis=0)
    return jnp.concatenate([prefix_addition_result, bulk_compactness[None] * velocity, energy[None], (bulk_compactness * passive)[None]], axis=0).astype(jnp.float32)


def set_ends(values, key, least, high):
    dims = values.shape
    index_at = [jax.random.randint(jax.random.fold_in(key, axis), (), 0, dims[axis]) for axis in range(len(dims))]
    values = values.at[tuple(index_at)].set(least)
    longest = dims.index(max(dims))
    index_at[longest] = (index_at[longest] + 1) % dims[longest]
    return values.at[tuple(index_at)].set(high)


def setup_inputs(seed: int = 0) -> dict:
    arg_keys = jax.random.split(jax.random.key(seed), 6)
    preserved_vector = draw_preserved_vector(jax.random.fold_in(arg_keys[5], 71), 0)
    nasa_table = draw_nasa_table(jax.random.fold_in(arg_keys[5], 71), 0)
    gas_constant = draw_gas_constant(jax.random.fold_in(arg_keys[5], 71), 0)
    species_index = draw_species_index(jax.random.fold_in(arg_keys[5], 71), 0)
    face_kind = set_ends(jax.random.randint(arg_keys[4], (N_GX, N_GY, 2), 0, 2), jax.random.fold_in(arg_keys[4], 1), 0, 1).astype(jnp.int32)
    return {"preserved_vector": preserved_vector, "nasa_table": nasa_table, "gas_constant": gas_constant, "species_index": species_index, "face_kind": face_kind}


EPSILON = 1e-06
COURANT = 0.8

def column(vector, trailing_sizes):
    return vector.reshape((vector.shape[0],) + (1,) * trailing_sizes)

def caloric_fitted_curves_table(nasa_table_weights, kelvin_reading):
    trailing_sizes = kelvin_reading.ndim
    columns = [column(nasa_table_weights[:, degree], trailing_sizes) for degree in range(6)]
    replicated_layer = kelvin_reading[None]
    caloric_quotient = columns[0] + replicated_layer * (columns[1] + replicated_layer * (columns[2] + replicated_layer * (columns[3] + replicated_layer * columns[4])))
    chemical_heat_content = columns[5] + replicated_layer * (columns[0] + replicated_layer * (columns[1] / 2.0 + replicated_layer * (columns[2] / 3.0 + replicated_layer * (columns[3] / 4.0 + replicated_layer * columns[4] / 5.0))))
    return (caloric_quotient, chemical_heat_content)

def solve_for_kelvin(preserved_vector_lines, nasa_table_weights, component_kind_r_factor):
    prefix_addition_result = preserved_vector_lines[:NS]
    bulk_compactness = lax.optimization_barrier(jnp.sum(prefix_addition_result, axis=0))
    momentum = preserved_vector_lines[NS:NS + 3]
    caloric_content_inner = preserved_vector_lines[NS + 3] - 0.5 * lax.optimization_barrier(jnp.sum(momentum * momentum, axis=0)) / bulk_compactness
    blend_stack_lane = column(component_kind_r_factor, bulk_compactness.ndim)
    kelvin_reading = jnp.ones_like(bulk_compactness)
    for iteration in range(NEWTON):
        caloric_quotient, chemical_heat_content = caloric_fitted_curves_table(nasa_table_weights, kelvin_reading)
        solver_misfit = lax.optimization_barrier(jnp.sum(prefix_addition_result * blend_stack_lane * (chemical_heat_content - kelvin_reading[None]), axis=0)) - caloric_content_inner
        tangent_steepness_fn = lax.optimization_barrier(jnp.sum(prefix_addition_result * blend_stack_lane * (caloric_quotient - 1.0), axis=0))
        kelvin_reading = kelvin_reading - solver_misfit / tangent_steepness_fn
    return kelvin_reading

def nasa_fitted_monomials(preserved_vector_lines, kelvin_reading, nasa_table_weights, component_kind_r_factor):
    prefix_addition_result = preserved_vector_lines[:NS]
    bulk_compactness = lax.optimization_barrier(jnp.sum(prefix_addition_result, axis=0))
    momentum = preserved_vector_lines[NS:NS + 3]
    doubled_norm_motion = lax.optimization_barrier(jnp.sum(momentum * momentum, axis=0)) / (bulk_compactness * bulk_compactness)
    blend_stack_lane = column(component_kind_r_factor, bulk_compactness.ndim)
    caloric_quotient, chemical_heat_content = caloric_fitted_curves_table(nasa_table_weights, kelvin_reading)
    caloric_tiers = blend_stack_lane * (chemical_heat_content - kelvin_reading[None])
    averaged_mixing_law_r = lax.optimization_barrier(jnp.sum(prefix_addition_result * blend_stack_lane, axis=0))
    thrust_load_quiet = averaged_mixing_law_r * kelvin_reading
    heat_quotient_decrement = averaged_mixing_law_r / lax.optimization_barrier(jnp.sum(prefix_addition_result * blend_stack_lane * (caloric_quotient - 1.0), axis=0))
    sound_speed = jnp.sqrt((1.0 + heat_quotient_decrement) * thrust_load_quiet / bulk_compactness)
    force_spatial_jump = blend_stack_lane * kelvin_reading[None] - heat_quotient_decrement[None] * caloric_tiers + 0.5 * heat_quotient_decrement[None] * doubled_norm_motion[None]
    return jnp.concatenate([thrust_load_quiet[None], heat_quotient_decrement[None], sound_speed[None], force_spatial_jump], axis=0)

def reconstruct(values):
    value_zero, value_one, value_two, value_three, value_four = values
    candidate_zero = (2.0 * value_zero - 7.0 * value_one + 11.0 * value_two) / 6.0
    candidate_one = (-value_one + 5.0 * value_two + 2.0 * value_three) / 6.0
    candidate_two = (2.0 * value_two + 5.0 * value_three - value_four) / 6.0
    curve_zero = value_zero - 2.0 * value_one + value_two
    slope_zero = value_zero - 4.0 * value_one + 3.0 * value_two
    curve_one = value_one - 2.0 * value_two + value_three
    slope_one = value_one - value_three
    curve_two = value_two - 2.0 * value_three + value_four
    slope_two = 3.0 * value_two - 4.0 * value_three + value_four
    smooth_zero = 13.0 / 12.0 * curve_zero * curve_zero + 0.25 * slope_zero * slope_zero
    smooth_one = 13.0 / 12.0 * curve_one * curve_one + 0.25 * slope_one * slope_one
    smooth_two = 13.0 / 12.0 * curve_two * curve_two + 0.25 * slope_two * slope_two
    weight_zero = 0.1 / ((EPSILON + smooth_zero) * (EPSILON + smooth_zero))
    weight_one = 0.6 / ((EPSILON + smooth_one) * (EPSILON + smooth_one))
    weight_two = 0.3 / ((EPSILON + smooth_two) * (EPSILON + smooth_two))
    return (weight_zero * candidate_zero + weight_one * candidate_one + weight_two * candidate_two) / (weight_zero + weight_one + weight_two)

def window(array, offset, count, array_axis):
    return lax.slice_in_dim(array, offset, offset + count, axis=array_axis)

def direction_rate(preserved_vector_lines, cell_coef, array_axis, normal, speed):
    cells = preserved_vector_lines.shape[array_axis] - 6
    faces = cells + 1
    bulk_compactness = lax.optimization_barrier(jnp.sum(preserved_vector_lines[:NS], axis=0))
    fractions = preserved_vector_lines[:NS] / bulk_compactness[None]
    velocity = preserved_vector_lines[NS:NS + 3] / bulk_compactness[None]
    passive = preserved_vector_lines[NS + 4:NS + 5] / bulk_compactness[None]
    thrust_load_quiet = cell_coef[0]
    normal_speed = velocity[normal]
    carried = preserved_vector_lines * normal_speed[None]
    flux_rows = [carried[:NS]]
    for component in range(3):
        if component == normal:
            flux_rows.append((carried[NS + component] + thrust_load_quiet)[None])
        else:
            flux_rows.append(carried[NS + component][None])
    flux_rows.append((carried[NS + 3] + thrust_load_quiet * normal_speed)[None])
    flux_rows.append(carried[NS + 4][None])
    physical = jnp.concatenate(flux_rows, axis=0)
    upwind = 0.5 * (physical + speed * preserved_vector_lines)
    downwind = 0.5 * (physical - speed * preserved_vector_lines)

    def average(array):
        return 0.5 * (window(array, 2, faces, array_axis) + window(array, 3, faces, array_axis))
    mean_frac = average(fractions)
    mean_vel = average(velocity)
    mean_passive = average(passive)[0]
    mean_gamma = average(cell_coef[1:2])[0]
    mean_sound = average(cell_coef[2:3])[0]
    mean_slopes = average(cell_coef[3:])
    mean_square = lax.optimization_barrier(jnp.sum(mean_vel * mean_vel, axis=0))
    mean_enthalpy = (mean_sound * mean_sound - lax.optimization_barrier(jnp.sum(mean_frac * mean_slopes, axis=0))) / mean_gamma + mean_square
    inverse = 1.0 / (mean_sound * mean_sound)
    tangents = [component for component in range(3) if component != normal]

    def project(vector):
        total = lax.optimization_barrier(jnp.sum(vector[:NS], axis=0))
        pressure_jump = lax.optimization_barrier(jnp.sum(mean_slopes * vector[:NS], axis=0)) - mean_gamma * lax.optimization_barrier(jnp.sum(mean_vel * vector[NS:NS + 3], axis=0)) + mean_gamma * vector[NS + 3]
        normal_jump = vector[NS + normal] - mean_vel[normal] * total
        scaled = pressure_jump * inverse
        slower = 0.5 * (pressure_jump - mean_sound * normal_jump) * inverse
        faster = 0.5 * (pressure_jump + mean_sound * normal_jump) * inverse
        species = vector[:NS] - mean_frac * scaled[None]
        first_shear = vector[NS + tangents[0]] - mean_vel[tangents[0]] * total
        second_shear = vector[NS + tangents[1]] - mean_vel[tangents[1]] * total
        scalar_wave = vector[NS + 4] - mean_passive * scaled
        return jnp.concatenate([slower[None], species, first_shear[None], second_shear[None], faster[None], scalar_wave[None]], axis=0)
    rising = reconstruct([project(window(upwind, offset, faces, array_axis)) for offset in (0, 1, 2, 3, 4)])
    falling = reconstruct([project(window(downwind, offset, faces, array_axis)) for offset in (5, 4, 3, 2, 1)])
    amplitude = rising + falling
    slower = amplitude[0]
    species = amplitude[1:NS + 1]
    first_shear = amplitude[NS + 1]
    second_shear = amplitude[NS + 2]
    faster = amplitude[NS + 3]
    scalar_wave = amplitude[NS + 4]
    species_total = lax.optimization_barrier(jnp.sum(species, axis=0))
    acoustic = slower + faster
    normal_vel = mean_vel[normal]
    momentum_rows = []
    for component in range(3):
        if component == normal:
            momentum_rows.append((normal_vel - mean_sound) * slower + (normal_vel + mean_sound) * faster + normal_vel * species_total)
        elif component == tangents[0]:
            momentum_rows.append(mean_vel[component] * (acoustic + species_total) + first_shear)
        else:
            momentum_rows.append(mean_vel[component] * (acoustic + species_total) + second_shear)
    energy_row = (mean_enthalpy - normal_vel * mean_sound) * slower + (mean_enthalpy + normal_vel * mean_sound) * faster + lax.optimization_barrier(jnp.sum((mean_square[None] - mean_slopes / mean_gamma[None]) * species, axis=0)) + mean_vel[tangents[0]] * first_shear + mean_vel[tangents[1]] * second_shear
    face_flux = jnp.concatenate([mean_frac * acoustic[None] + species, jnp.stack(momentum_rows, axis=0), energy_row[None], (mean_passive * acoustic + scalar_wave)[None]], axis=0)
    return window(face_flux, 0, cells, array_axis) - window(face_flux, 1, cells, array_axis)

def wall_pad(payload, lower_kind, upper_kind):
    rows_count = payload.shape[0]
    sign_flips = jnp.where(jnp.arange(rows_count) == NS + 2, -1.0, 1.0).astype(payload.dtype).reshape((rows_count, 1, 1, 1))
    lower_copy = jnp.concatenate([payload[..., :1]] * 3, axis=3)
    upper_copy = jnp.concatenate([payload[..., -1:]] * 3, axis=3)
    lower_mirror = payload[..., 2::-1] * sign_flips
    upper_mirror = payload[..., :-4:-1] * sign_flips
    lower_ghost = jnp.where(lower_kind == 1, lower_mirror, lower_copy)
    upper_ghost = jnp.where(upper_kind == 1, upper_mirror, upper_copy)
    return jnp.concatenate([lower_ghost, payload, upper_ghost], axis=3)

def reference(preserved_vector, nasa_table, gas_constant, species_index, face_kind):
    nasa_table_weights = nasa_table[species_index]
    component_kind_r_factor = gas_constant[species_index]
    block_ids = jnp.arange(N_GX, dtype=jnp.int32)

    def cell_block(block_id):
        patch_region = lax.dynamic_slice_in_dim(preserved_vector, (block_id * CX).astype(jnp.int32), CX, 1)
        kelvin_reading = solve_for_kelvin(patch_region, nasa_table_weights, component_kind_r_factor)
        patch_multiplier = nasa_fitted_monomials(patch_region, kelvin_reading, nasa_table_weights, component_kind_r_factor)
        bulk_compactness = lax.optimization_barrier(jnp.sum(patch_region[:NS], axis=0))
        velocity = patch_region[NS:NS + 3] / bulk_compactness[None]
        local_speed = lax.optimization_barrier(jnp.max(jnp.abs(velocity) + patch_multiplier[2][None], axis=(1, 2, 3)))
        return (patch_multiplier, local_speed)
    coef_blocks, speed_blocks = lax.map(cell_block, block_ids)
    cell_coef = jnp.transpose(coef_blocks, (1, 0, 2, 3, 4)).reshape((NS + 3, NX, NY, NZ))
    speeds = lax.optimization_barrier(jnp.max(speed_blocks, axis=0))

    def rate_block(inputs):
        block_id, kinds = inputs
        rows_index = (block_id * CX - 3 + jnp.arange(CX + 6, dtype=jnp.int32)) % NX
        state_x = jnp.take(preserved_vector, rows_index, axis=1)
        coef_x = jnp.take(cell_coef, rows_index, axis=1)
        rate = direction_rate(state_x, coef_x, 1, 0, speeds[0])
        state_mid = state_x[:, 3:3 + CX]
        coef_mid = coef_x[:, 3:3 + CX]
        state_y = jnp.concatenate([state_mid[:, :, -3:], state_mid, state_mid[:, :, :3]], axis=2)
        coef_y = jnp.concatenate([coef_mid[:, :, -3:], coef_mid, coef_mid[:, :, :3]], axis=2)
        rate = rate + direction_rate(state_y, coef_y, 2, 1, speeds[1])
        lower_kind = jnp.repeat(kinds[:, 0], CY).reshape((1, 1, NY, 1))
        upper_kind = jnp.repeat(kinds[:, 1], CY).reshape((1, 1, NY, 1))
        padded_z = wall_pad(jnp.concatenate([state_mid, coef_mid], axis=0), lower_kind, upper_kind)
        rate = rate + direction_rate(padded_z[:NVAR], padded_z[NVAR:], 3, 2, speeds[2])
        return rate
    rate_blocks = lax.map(rate_block, (block_ids, face_kind))
    rate = jnp.transpose(rate_blocks, (1, 0, 2, 3, 4)).reshape((NVAR, NX, NY, NZ))
    return COURANT / jnp.sum(speeds) * rate
```

```python
import functools

import jax
import jax.numpy as jnp
from jax import lax
from jax.experimental import pallas as pl
from jax.experimental.pallas import tpu as pltpu
from jax.sharding import PartitionSpec as P

NS = 9
NVAR = 14
EPSILON = 1e-06
COURANT = 0.8
TOTAL = NVAR
PRIMS = 24
VEL, PASSIVE, GAMMA, SOUND, SLOPES = 9, 12, 13, 14, 15
TABLE = 7 * NS


def fill_table(nasa_ref, gas_ref, index_ref, table_ref):
    for i in range(NS):
        row = index_ref[i]
        gas = gas_ref[row]
        values = [
            gas,
            gas * nasa_ref[5, row],
            gas * (nasa_ref[0, row] - 1.0),
            gas * nasa_ref[1, row] * (1.0 / 2.0),
            gas * nasa_ref[2, row] * (1.0 / 3.0),
            gas * nasa_ref[3, row] * (1.0 / 4.0),
            gas * nasa_ref[4, row] * (1.0 / 5.0),
        ]
        for n, value in enumerate(values):
            table_ref[n * NS + i] = jnp.full(table_ref.shape[1:], value, jnp.float32)


def tree(terms):
    terms = list(terms)
    while len(terms) > 1:
        terms = [a + b for a, b in zip(terms[::2], terms[1::2])] + (
            [terms[-1]] if len(terms) % 2 else []
        )
    return terms[0]


def thermo(u, table_ref):
    rho = tree(u[:NS])
    inverse = 1.0 / rho
    vel = [m * inverse for m in u[NS : NS + 3]]
    square = tree([v * v for v in vel])
    inner = u[NS + 3] - 0.5 * tree([v * m for v, m in zip(vel, u[NS : NS + 3])])
    mix = [tree([u[i] * table_ref[n * NS + i] for i in range(NS)]) for n in range(7)]
    gas, m6, m1, m2, m3, m4, m5 = mix
    c2, c3, c4, c5 = 2.0 * m2, 3.0 * m3, 4.0 * m4, 5.0 * m5
    temp = 1.0 - (tree([m6, m1, m2, m3, m4, m5]) - inner) / tree([m1, c2, c3, c4, c5])

    def heat(t):
        return m1 + t * (c2 + t * (c3 + t * (c4 + t * c5)))

    energy = m6 + temp * (m1 + temp * (m2 + temp * (m3 + temp * (m4 + temp * m5))))
    temp = temp - (energy - inner) / heat(temp)
    pressure = temp * gas
    gamma = gas / heat(temp)
    sound = jnp.sqrt((1.0 + gamma) * pressure * inverse)
    return inverse, vel, square, temp, pressure, gamma, sound


def slopes_of(temp, gamma, square, table_ref):
    kinetic = 0.5 * gamma * square
    result = []
    for i in range(NS):
        k = [table_ref[n * NS + i] for n in range(7)]
        e = k[1] + temp * (k[2] + temp * (k[3] + temp * (k[4] + temp * (k[5] + temp * k[6]))))
        result.append(k[0] * temp - gamma * e + kinetic)
    return result


def reciprocal(x):
    return pl.reciprocal(x, approx=True)


def correction(d):
    d0, d1, d2, d3 = d
    e0, e1, e2 = d1 - d0, d2 - d1, d3 - d2
    h1, h2 = 0.75 * d1, 0.75 * d2
    near, far = h1 * d1 + 0.75 * EPSILON, h2 * d2 + 0.75 * EPSILON
    r0 = reciprocal(e0 * (e0 + h1) + near)
    r1 = reciprocal(e1 * (e1 + h1) + near)
    r2 = reciprocal(e2 * (e2 - h2) + far)
    a = r0 * r0 * (1.0 / 3.0)
    b = r1 * r1
    c = r2 * r2
    g0, g2 = e0 - e1, e1 - e2
    return (a * (g0 + g0) + c * g2) * reciprocal(a + c + (b + b))


def face(normal, up, down, mean, linear, put):
    phi = [mean(SLOPES + i) for i in range(NS)]
    vel = [mean(VEL + i) for i in range(3)]
    gamma, sound = mean(GAMMA), mean(SOUND)
    inv = 1.0 / sound
    inv2, half_inv = inv * inv, 0.5 * inv
    tangents = [t for t in range(3) if t != normal]
    sigma, slow, fast = ([], []), ([], []), ([], [])
    shear = [([], []), ([], [])]
    for side, get in enumerate((up, down)):
        for k in range(4):
            s = get(TOTAL, k)
            m = [get(NS + i, k) for i in range(3)]
            dp = tree([phi[i] * get(i, k) for i in range(NS)]) + gamma * (
                get(NS + 3, k) - tree([vel[i] * m[i] for i in range(3)])
            )
            scaled = dp * inv2
            jump = (m[normal] - vel[normal] * s) * half_inv
            half = 0.5 * scaled
            sigma[side].append(scaled)
            slow[side].append(half - jump)
            fast[side].append(half + jump)
            for n, t in enumerate(tangents):
                shear[n][side].append(m[t] - vel[t] * s)

    def both(pair):
        return correction(pair[0]) - correction(pair[1])

    slower, faster = both(slow), both(fast)
    shears = [both(pair) for pair in shear]
    acoustic = slower + faster
    total, weighted, blend = None, None, None
    for i in range(NS):
        y = mean(i)
        amp = both(
            (
                [up(i, k) - y * sigma[0][k] for k in range(4)],
                [down(i, k) - y * sigma[1][k] for k in range(4)],
            )
        )
        put(i, linear(i) + y * acoustic + amp)
        total = amp if i == 0 else total + amp
        weighted = phi[i] * amp if i == 0 else weighted + phi[i] * amp
        blend = phi[i] * y if i == 0 else blend + phi[i] * y
    z = mean(PASSIVE)
    amp = both(
        (
            [up(NS + 4, k) - z * sigma[0][k] for k in range(4)],
            [down(NS + 4, k) - z * sigma[1][k] for k in range(4)],
        )
    )
    put(NS + 4, linear(NS + 4) + z * acoustic + amp)
    mass = acoustic + total
    swing = sound * (faster - slower)
    put(NS + normal, linear(NS + normal) + vel[normal] * mass + swing)
    for n, t in enumerate(tangents):
        put(NS + t, linear(NS + t) + vel[t] * mass + shears[n])
    square = tree([v * v for v in vel])
    energy = (
        square * mass
        + ((sound * sound - blend) * acoustic - weighted) / gamma
        + vel[normal] * swing
        + vel[tangents[0]] * shears[0]
        + vel[tangents[1]] * shears[1]
    )
    put(NS + 3, linear(NS + 3) + energy)


def fill_cells(u, i, table_ref, prim_ref):
    inverse, vel, square, temp, pressure, gamma, sound = thermo(u, table_ref)
    for k in range(NS):
        prim_ref[k, i] = u[k] * inverse
    for k in range(3):
        prim_ref[VEL + k, i] = vel[k]
    prim_ref[PASSIVE, i] = u[NS + 4] * inverse
    prim_ref[GAMMA, i] = gamma
    prim_ref[SOUND, i] = sound
    for k, value in enumerate(slopes_of(temp, gamma, square, table_ref)):
        prim_ref[SLOPES + k, i] = value
    prim_ref[PRIMS, i] = pressure


def fill_split(u, i, normal, alpha, prim_ref, up_ref, down_ref):
    speed = prim_ref[VEL + normal, i]
    push = 0.5 * prim_ref[PRIMS, i]
    half = 0.5 * speed
    lean = 0.5 * alpha
    plus, minus = half + lean, half - lean
    for ref, factor in ((up_ref, plus), (down_ref, minus)):
        for k in range(NVAR):
            value = u[k] * factor
            if k == NS + normal:
                value = value + push
            if k == NS + 3:
                value = value + push * speed
            ref[k, i] = value
        ref[TOTAL, i] = tree(u[:NS]) * factor


MESH = pl.DeviceIdType.MESH


def fused(
    size_x, size_y,
    nasa_hbm, gas_hbm, index_hbm, kind_hbm, flat_ref, planes_ref, source_ref, out_ref,
    nasa_ref, gas_ref, index_ref, kind_ref,
    x_ref, hx_ref, hy_ref, mine_ref, slots_ref,
    table_ref, prim_ref, turn_ref, up_ref, down_ref, dup_ref, ddown_ref,
    fx_ref, fz_ref, acc_ref, edge_ref, fy_ref, s0_ref, s1_ref, s2_ref, s3_ref,
    load_sem, param_sem, small_send, small_recv, big_send, big_recv,
):
    load = pltpu.make_async_copy(flat_ref, x_ref, load_sem)
    load.start()
    params = [
        pltpu.make_async_copy(source, target, param_sem.at[n])
        for n, (source, target) in enumerate(
            (
                (nasa_hbm, nasa_ref),
                (gas_hbm, gas_ref),
                (index_hbm, index_ref),
                (kind_hbm, kind_ref),
            )
        )
    ]
    for copy in params:
        copy.start()
    gx, gy = lax.axis_index("gx"), lax.axis_index("gy")
    nx, ny = planes_ref.shape[1], planes_ref.shape[2]

    def there(ox, oy):
        return (lax.rem(gx + ox, size_x), lax.rem(gy + oy, size_y))

    others = [(ox, oy) for ox in range(size_x) for oy in range(size_y) if ox or oy]
    barrier = pltpu.get_barrier_semaphore()
    for ox, oy in others:
        pl.semaphore_signal(barrier, inc=1, device_id=there(ox, oy), device_id_type=MESH)
    for copy in params:
        copy.wait()
    fill_table(nasa_ref, gas_ref, index_ref, table_ref)
    load.wait()

    lanes = x_ref.shape[1]
    tile = (8, lanes)
    block = nx * ny

    def own(r, x):
        return x_ref[pl.ds(pl.multiple_of(r * block + x * 8, 8), 8), :]

    def turned(r, y):
        return x_ref[pl.ds(r * block + y, 8, stride=8), :]

    def differences(first, last, split):
        up_ref, down_ref, dup_ref, ddown_ref = split

        def step(i, _):
            for k in range(NVAR + 1):
                dup_ref[k, i] = up_ref[k, i + 1] - up_ref[k, i]
                ddown_ref[k, i] = down_ref[k, i + 1] - down_ref[k, i]
            return 0

        lax.fori_loop(first, last, step, 0)

    def faces_across(normal, first, last, prim_ref, split, flux_ref):
        up_ref, down_ref, dup_ref, ddown_ref = split

        def step(i, _):
            def linear(r):
                here = up_ref[r, i + 2] + down_ref[r, i + 3]
                ahead = dup_ref[r, i + 2] - ddown_ref[r, i + 2]
                return 6.0 * here + (ahead + ahead) + (dup_ref[r, i + 1] - ddown_ref[r, i + 3])

            def put(r, value):
                flux_ref[r, i] = value

            face(
                normal,
                lambda r, k: dup_ref[r, i + k],
                lambda r, k: ddown_ref[r, i + 4 - k],
                lambda q: 0.5 * (prim_ref[q, i + 2] + prim_ref[q, i + 3]),
                linear,
                put,
            )
            return 0

        lax.fori_loop(first, last, step, 0)

    def y_halo_tile(side, r, k):
        return hy_ref[side, r, :, k, 0, :]

    def cells_halo(normal, prims, split, read):
        def step(k, _):
            for side, base in ((0, 0), (1, 11)):
                u = [read(side, r, k) for r in range(NVAR)]
                fill_cells(u, k + base, table_ref, prims)
                fill_split(u, k + base, normal, alphas[normal], prims, *split[:2])
            return 0

        lax.fori_loop(0, 3, step, 0)

    def split_own(normal, prims, split, read):
        def step(n, _):
            u = [read(r, n) for r in range(NVAR)]
            fill_split(u, n + 3, normal, alphas[normal], prims, *split[:2])
            return 0

        lax.fori_loop(0, 8, step, 0)

    def y_prims(y, _):
        fill_cells([turned(r, y) for r in range(NVAR)], y + 3, table_ref, turn_ref)
        return 0

    lane = lax.broadcasted_iota(jnp.int32, tile, 1)

    width = 16
    spot = lane % width
    reach = spot - 3
    low_wall, high_wall = kind_ref[0] == 1, kind_ref[1] == 1
    low = jnp.where(reach < 0, jnp.where(low_wall, -1 - reach, 0), reach)
    beyond = spot - 13
    high = jnp.where(
        beyond >= 0,
        jnp.where(high_wall, lanes - 1 - beyond, lanes - 1),
        lanes + beyond,
    )
    source = jnp.where(spot < 8, low, high)
    mirrored = ((spot < 3) & low_wall) | ((spot > 12) & high_wall)
    sign = jnp.where(mirrored, -1.0, 1.0)
    group = lane // width

    def gather(values, index):
        return jnp.take_along_axis(values, index, axis=1)

    def z_edge(x, _):
        for r in range(NVAR):
            value = gather(own(r, x), source)
            if r == NS + 2:
                value = value * sign
            edge_ref[r] = jnp.where(group == x, value, edge_ref[r])
        return 0

    def roll(values, shift):
        return values if shift % lanes == 0 else pltpu.roll(values, shift % lanes, 1)

    def z_split(u, i):
        fill_split(u, i, 2, alphas[2], prim_ref, up_ref, down_ref)
        for k in range(NVAR + 1):
            dup_ref[k, i] = roll(up_ref[k, i], -1) - up_ref[k, i]
            ddown_ref[k, i] = roll(down_ref[k, i], -1) - down_ref[k, i]

    def z_own(x, _):
        u = [own(r, x) for r in range(NVAR)]
        z_split(u, x + 3)
        return 0

    def z_faces(x, _):
        i = jnp.where(x == 8, 14, x + 3)

        def linear(r):
            here = up_ref[r, i] + roll(down_ref[r, i], -1)
            ahead = dup_ref[r, i] - ddown_ref[r, i]
            return 6.0 * here + (ahead + ahead) + (
                roll(dup_ref[r, i], 1) - roll(ddown_ref[r, i], -1)
            )

        def mean(q):
            value = prim_ref[q, i]
            return 0.5 * (value + roll(value, -1))

        def put(r, value):
            fz_ref[r, x] = value

        face(
            2,
            lambda r, k: roll(dup_ref[r, i], 2 - k),
            lambda r, k: roll(ddown_ref[r, i], k - 2),
            mean,
            linear,
            put,
        )
        return 0

    def x_prims(x, best):
        u = [own(r, x) for r in range(NVAR)]
        fill_cells(u, x + 3, table_ref, prim_ref)
        sound = prim_ref[SOUND, x + 3]
        return tuple(
            jnp.maximum(b, jnp.abs(prim_ref[VEL + d, x + 3]) + sound) for d, b in enumerate(best)
        )

    zero = jnp.zeros(tile, jnp.float32)
    best = lax.fori_loop(0, 8, x_prims, (zero, zero, zero))
    best = [jnp.max(b, axis=(0, 1), keepdims=True) for b in best]
    column = lax.broadcasted_iota(jnp.int32, (1, lanes), 1)
    mine_ref[...] = jnp.where(column == 0, best[0], jnp.where(column == 1, best[1], best[2]))
    pl.semaphore_wait(barrier, len(others))

    peers = []
    for n, (ox, oy) in enumerate(others):
        copy = pltpu.make_async_remote_copy(
            src_ref=mine_ref,
            dst_ref=slots_ref.at[n],
            send_sem=small_send.at[n],
            recv_sem=small_recv.at[n],
            device_id=there(ox, oy),
            device_id_type=MESH,
        )
        copy.start()
        peers.append(copy)
    halos = []
    for n, (origin, target, device) in enumerate(
        (
            (planes_ref.at[:, pl.ds(nx - 3, 3)], hx_ref.at[0], there(1, 0)),
            (planes_ref.at[:, pl.ds(0, 3)], hx_ref.at[1], there(size_x - 1, 0)),
            (source_ref.at[:, :, pl.ds(ny - 3, 3)], hy_ref.at[0], there(0, 1)),
            (source_ref.at[:, :, pl.ds(0, 3)], hy_ref.at[1], there(0, size_y - 1)),
        )
    ):
        copy = pltpu.make_async_remote_copy(
            src_ref=origin,
            dst_ref=target,
            send_sem=big_send.at[n],
            recv_sem=big_recv.at[n],
            device_id=device,
            device_id_type=MESH,
        )
        copy.start()
        halos.append(copy)

    for r in range(NVAR):
        edge_ref[r] = zero
    lax.fori_loop(0, 8, z_edge, 0)
    fill_cells([edge_ref[r] for r in range(NVAR)], 14, table_ref, prim_ref)
    lax.fori_loop(0, 8, y_prims, 0)

    for copy in peers:
        copy.wait()
    value = mine_ref[...]
    for n in range(len(others)):
        value = jnp.maximum(value, slots_ref[n])
    alphas = [
        jnp.broadcast_to(
            jnp.max(jnp.where(column == d, value, 0.0), axis=1, keepdims=True), tile
        )
        for d in range(3)
    ]

    z_split([edge_ref[r] for r in range(NVAR)], 14)
    lax.fori_loop(0, 8, z_own, 0)
    lax.fori_loop(0, 9, z_faces, 0)

    splits = (up_ref, down_ref, dup_ref, ddown_ref), (s0_ref, s1_ref, s2_ref, s3_ref)
    plans = (
        (1, turn_ref, splits[1], turned, y_halo_tile, fy_ref, halos[2:]),
        (0, prim_ref, splits[0], own, lambda side, r, k: hx_ref[side, r, k], fx_ref, halos[:2]),
    )
    for normal, prims, split, read, _, flux, _ in plans:
        split_own(normal, prims, split, read)
        differences(3, 10, split)
        faces_across(normal, 3, 6, prims, split, flux)
    for normal, prims, split, _, read, flux, copies in plans:
        for copy in copies:
            copy.wait()
        cells_halo(normal, prims, split, read)
        differences(0, 3, split)
        differences(10, 13, split)
        faces_across(normal, 0, 3, prims, split, flux)
        faces_across(normal, 6, 9, prims, split, flux)

    def y_rate(y, _):
        for r in range(NVAR):
            acc_ref[pl.ds(r * block + y, 8, stride=8), :] = fy_ref[r, y + 1] - fy_ref[r, y]
        return 0

    lax.fori_loop(0, 8, y_rate, 0)

    scale = (-COURANT / 6.0) / (alphas[0] + alphas[1] + alphas[2])
    near = jnp.where(lane < 2, lane + 3, lane - lanes + 13)
    patched = (lane < 2) | (lane > lanes - 4)

    def finish(x, _):
        first = jnp.clip(width * x + near, 0, lanes - 1)
        below = jnp.full(tile, width * x + 2, jnp.int32)
        for r in range(NVAR):
            edges = fz_ref[r, 8]
            upper = jnp.where(patched, gather(edges, first), fz_ref[r, x])
            lower = jnp.where(lane == 0, gather(edges, below), roll(upper, 1))
            rows = pl.ds(pl.multiple_of(r * block + x * 8, 8), 8)
            rate = (upper - lower) + (fx_ref[r, x + 1] - fx_ref[r, x]) + acc_ref[rows, :]
            out_ref[rows, :] = scale * rate
        return 0

    lax.fori_loop(0, 8, finish, 0)


def shards(preserved_vector, nasa_table, gas_constant, species_index, face_kind):
    _, nx, ny, lanes = preserved_vector.shape
    size_x, size_y = lax.axis_size("gx"), lax.axis_size("gy")
    flat = preserved_vector.reshape(NVAR * nx * ny, lanes)
    hbm = pl.BlockSpec(memory_space=pltpu.HBM)
    dma = pltpu.SemaphoreType.DMA

    def buffer(*shape):
        return pltpu.VMEM(shape + (8, lanes), jnp.float32)

    out = pl.pallas_call(
        functools.partial(fused, size_x, size_y),
        out_shape=jax.ShapeDtypeStruct(flat.shape, jnp.float32),
        in_specs=[hbm] * 7,
        out_specs=pl.BlockSpec(memory_space=pltpu.VMEM),
        scratch_shapes=[
            pltpu.SMEM(nasa_table.T.shape, jnp.float32),
            pltpu.SMEM(gas_constant.shape, jnp.float32),
            pltpu.SMEM(species_index.shape, jnp.int32),
            pltpu.SMEM((2,), jnp.int32),
            pltpu.VMEM(flat.shape, jnp.float32),
            buffer(2, NVAR, 3),
            pltpu.VMEM((2, NVAR, nx, 3, 1, lanes), jnp.float32),
            pltpu.VMEM((1, lanes), jnp.float32),
            pltpu.VMEM((size_x * size_y - 1, 1, lanes), jnp.float32),
            buffer(TABLE),
            buffer(PRIMS + 1, 15),
            buffer(PRIMS + 1, 15),
            buffer(NVAR + 1, 15),
            buffer(NVAR + 1, 15),
            buffer(NVAR + 1, 15),
            buffer(NVAR + 1, 15),
            buffer(NVAR, 9),
            buffer(NVAR, 9),
            pltpu.VMEM(flat.shape, jnp.float32),
            buffer(NVAR),
            buffer(NVAR, 9),
            *[buffer(NVAR + 1, 15) for _ in range(4)],
            dma(()),
            dma((4,)),
            dma((size_x * size_y - 1,)),
            dma((size_x * size_y - 1,)),
            dma((4,)),
            dma((4,)),
        ],
        compiler_params=pltpu.CompilerParams(
            collective_id=0, has_side_effects=True, vmem_limit_bytes=20 * 1024 * 1024
        ),
        name="increment",
    )(
        nasa_table.T, gas_constant, species_index, face_kind.reshape(2), flat,
        preserved_vector, preserved_vector.reshape(NVAR, nx, ny, 1, lanes),
    )
    return out.reshape(preserved_vector.shape)


def solution(mesh):
    return jax.shard_map(
        shards,
        mesh=mesh,
        in_specs=(P(None, "gx", "gy", None), P(), P(), P(), P("gx", "gy", None)),
        out_specs=P(None, "gx", "gy", None),
        check_vma=False,
    )
```

```python
import functools

import jax
import jax.numpy as jnp
from jax import lax
from jax.experimental import pallas as pl
from jax.experimental.pallas import tpu as pltpu
from jax.sharding import PartitionSpec as P

NS = 9
NVAR = 14
EPSILON = 1e-06
COURANT = 0.8
TOTAL = NVAR
PRIMS = 24
VEL, PASSIVE, GAMMA, SOUND, SLOPES = 9, 12, 13, 14, 15
TABLE = 7 * NS
ORDER = ((0, 1, 2), (1, 0, 2), (2, 0, 1))
PARTS = 7
ROW = 2 * PARTS + 2
STEEP, ENTHALPY, SQUARE = 14, 23, 24
COEFS = 25
FACES = 9
MESH = pl.DeviceIdType.MESH


def fill_table(nasa_ref, gas_ref, index_ref, table_ref):
    for i in range(NS):
        row = index_ref[i]
        gas = gas_ref[row]
        values = [
            gas,
            gas * nasa_ref[5, row],
            gas * (nasa_ref[0, row] - 1.0),
            gas * nasa_ref[1, row] * (1.0 / 2.0),
            gas * nasa_ref[2, row] * (1.0 / 3.0),
            gas * nasa_ref[3, row] * (1.0 / 4.0),
            gas * nasa_ref[4, row] * (1.0 / 5.0),
        ]
        for n, value in enumerate(values):
            table_ref[n * NS + i] = jnp.full(table_ref.shape[1:], value, jnp.float32)


def tree(terms):
    terms = list(terms)
    while len(terms) > 1:
        terms = [a + b for a, b in zip(terms[::2], terms[1::2])] + (
            [terms[-1]] if len(terms) % 2 else []
        )
    return terms[0]


def thermo(u, table_ref):
    rho = tree(u[:NS])
    inverse = 1.0 / rho
    vel = [m * inverse for m in u[NS : NS + 3]]
    inner = u[NS + 3] - 0.5 * tree([v * m for v, m in zip(vel, u[NS : NS + 3])])
    mix = [tree([u[i] * table_ref[n * NS + i] for i in range(NS)]) for n in range(7)]
    gas, m6, m1, m2, m3, m4, m5 = mix
    c2, c3, c4, c5 = 2.0 * m2, 3.0 * m3, 4.0 * m4, 5.0 * m5
    temp = 1.0 - (tree([m6, m1, m2, m3, m4, m5]) - inner) / tree([m1, c2, c3, c4, c5])

    def heat(t):
        return m1 + t * (c2 + t * (c3 + t * (c4 + t * c5)))

    energy = m6 + temp * (m1 + temp * (m2 + temp * (m3 + temp * (m4 + temp * m5))))
    temp = temp - (energy - inner) / heat(temp)
    pressure = temp * gas
    gamma = gas / heat(temp)
    sound = jnp.sqrt((1.0 + gamma) * pressure * inverse)
    return inverse, vel, temp, pressure, gamma, sound


def slopes_of(temp, gamma, square, table_ref):
    kinetic = 0.5 * gamma * square
    result = []
    for i in range(NS):
        k = [table_ref[n * NS + i] for n in range(7)]
        e = k[1] + temp * (k[2] + temp * (k[3] + temp * (k[4] + temp * (k[5] + temp * k[6]))))
        result.append(k[0] * temp - gamma * e + kinetic)
    return result


def reciprocal(x):
    return pl.reciprocal(x, approx=True)


def correction(d1, d2, e0, e1, e2):
    h1, h2 = 0.75 * d1, 0.75 * d2
    near, far = h1 * d1 + 0.75 * EPSILON, h2 * d2 + 0.75 * EPSILON
    r0 = reciprocal(e0 * (e0 + h1) + near)
    r1 = reciprocal(e1 * (e1 + h1) + near)
    r2 = reciprocal(e2 * (e2 - h2) + far)
    a = r0 * r0 * (1.0 / 3.0)
    b = r1 * r1
    c = r2 * r2
    g0, g2 = e0 - e1, e1 - e2
    return (a * (g0 + g0) + c * g2) * reciprocal(a + c + (b + b))


def fused(
    size_x, size_y,
    nasa_hbm, gas_hbm, index_hbm, kind_hbm, flat_ref, planes_ref, out_ref,
    nasa_ref, gas_ref, index_ref, kind_ref,
    x_ref, z_ref, acc_ref, back_ref, hx_ref, sy_ref, hy_ref, mine_ref, slots_ref,
    table_ref, cache_ref, prim_ref, f_ref, u_ref, df_ref, du_ref,
    part_ref, coef_ref, alpha_ref, flux_ref,
    load_sem, param_sem, small_send, small_recv, big_send, big_recv,
):
    load = pltpu.make_async_copy(flat_ref, x_ref, load_sem)
    load.start()
    params = [
        pltpu.make_async_copy(origin, target, param_sem.at[n])
        for n, (origin, target) in enumerate(
            (
                (nasa_hbm, nasa_ref),
                (gas_hbm, gas_ref),
                (index_hbm, index_ref),
                (kind_hbm, kind_ref),
            )
        )
    ]
    for copy in params:
        copy.start()
    gx, gy = lax.axis_index("gx"), lax.axis_index("gy")
    nx, ny = planes_ref.shape[1], planes_ref.shape[2]
    lanes = x_ref.shape[1]
    tile = (8, lanes)
    block = nx * ny

    def there(ox, oy):
        return (lax.rem(gx + ox, size_x), lax.rem(gy + oy, size_y))

    others = [(ox, oy) for ox in range(size_x) for oy in range(size_y) if ox or oy]
    barrier = pltpu.get_barrier_semaphore()
    for ox, oy in others:
        pl.semaphore_signal(barrier, inc=1, device_id=there(ox, oy), device_id_type=MESH)
    for copy in params:
        copy.wait()
    fill_table(nasa_ref, gas_ref, index_ref, table_ref)
    load.wait()

    def own(r, x):
        return x_ref[pl.ds(pl.multiple_of(r * block + x * 8, 8), 8), :]

    def turned(r, y):
        return x_ref[pl.ds(r * block + y, 8, stride=8), :]

    def upright(r, t):
        return z_ref[pl.ds(r * block + t, 8, stride=8), :]

    def flow(d, p, u, vel, pressure):
        order = ORDER[d]
        speed = vel[order[0]]
        half, push = 0.5 * speed, 0.5 * pressure
        rows = list(range(NS)) + [NS + n for n in order] + [NS + 3, NS + 4]
        for k, r in enumerate(rows):
            value = u[r] * half
            if k == NS:
                value = value + push
            if k == NS + 3:
                value = value + push * speed
            f_ref[d, p, k] = value
            u_ref[d, p, k] = 0.5 * u[r]
        rho = tree(u[:NS])
        f_ref[d, p, TOTAL] = rho * half
        u_ref[d, p, TOTAL] = 0.5 * rho

    def cells(d, p, u, state):
        inverse, vel, temp, pressure, gamma, sound = state
        flow(d, p, u, vel, pressure)
        q = p - 2
        for k in range(NS):
            prim_ref[d, q, k] = u[k] * inverse
        for k in range(3):
            prim_ref[d, q, VEL + k] = vel[ORDER[d][k]]
        prim_ref[d, q, PASSIVE] = u[NS + 4] * inverse
        prim_ref[d, q, GAMMA] = gamma
        prim_ref[d, q, SOUND] = sound
        square = tree([v * v for v in vel])
        for k, value in enumerate(slopes_of(temp, gamma, square, table_ref)):
            prim_ref[d, q, SLOPES + k] = value

    def own_cells(d, read):
        def step(n, _):
            u = [read(r, n) for r in range(NVAR)]
            cells(d, n + 3, u, thermo(u, table_ref))
            return 0

        lax.fori_loop(0, 8, step, 0)

    def halo_cells(d, read):
        for side, k, p in ((0, 2, 2), (1, 0, 11)):
            u = [read(side, r, k) for r in range(NVAR)]
            cells(d, p, u, thermo(u, table_ref))

        def step(k, _):
            for side, base in ((0, 0), (1, 11)):
                u = [read(side, r, k + side) for r in range(NVAR)]
                _, vel, _, pressure, _, _ = thermo(u, table_ref)
                flow(d, k + side + base, u, vel, pressure)
            return 0

        lax.fori_loop(0, 2, step, 0)

    def differences(d, first, last):
        def step(p, _):
            for k in range(NVAR + 1):
                df_ref[d, p, k] = f_ref[d, p + 1, k] - f_ref[d, p, k]
                du_ref[d, p, k] = u_ref[d, p + 1, k] - u_ref[d, p, k]
            return 0

        lax.fori_loop(first, last, step, 0)

    def project(d, first, last, start):
        def step(i, _):
            g = i + (start - first)

            def mean(q):
                return 0.5 * (prim_ref[d, i, q] + prim_ref[d, i + 1, q])

            y = [mean(k) for k in range(NS)]
            vel = [mean(VEL + k) for k in range(3)]
            phi = [mean(SLOPES + k) for k in range(NS)]
            z, gamma, sound = mean(PASSIVE), mean(GAMMA), mean(SOUND)
            inv = 1.0 / sound
            inv2, half_inv = inv * inv, 0.5 * inv
            steep = 1.0 / gamma
            for k in range(NS):
                coef_ref[g, k] = y[k]
                coef_ref[g, STEEP + k] = phi[k] * steep
            for k in range(3):
                coef_ref[g, VEL + k] = vel[k]
            coef_ref[g, PASSIVE] = z
            coef_ref[g, GAMMA] = sound
            coef_ref[g, ENTHALPY] = (
                sound * sound - tree([a * b for a, b in zip(y, phi)])
            ) * steep
            coef_ref[g, SQUARE] = tree([v * v for v in vel])
            for half, ref in enumerate((df_ref, du_ref)):

                def keep(n, d5):
                    at = n * ROW + half * PARTS
                    for j in range(3):
                        part_ref[g, at + j] = d5[j + 1]
                    for j in range(4):
                        part_ref[g, at + 3 + j] = d5[j + 1] - d5[j]

                waves = [[] for _ in range(5)]
                for k in range(5):
                    s = ref[d, i + k, TOTAL]
                    m = [ref[d, i + k, NS + n] for n in range(3)]
                    dp = tree([phi[n] * ref[d, i + k, n] for n in range(NS)]) + gamma * (
                        ref[d, i + k, NS + 3] - tree([vel[n] * m[n] for n in range(3)])
                    )
                    scaled = dp * inv2
                    jump = (m[0] - vel[0] * s) * half_inv
                    middle = 0.5 * scaled
                    waves[0].append(scaled)
                    waves[1].append(middle - jump)
                    waves[2].append(m[1] - vel[1] * s)
                    waves[3].append(m[2] - vel[2] * s)
                    waves[4].append(middle + jump)
                for n in range(4):
                    keep(NS + n, waves[n + 1])
                for n, share in enumerate(y):
                    keep(n, [ref[d, i + k, n] - share * waves[0][k] for k in range(5)])
                keep(NS + 4, [ref[d, i + k, NS + 4] - z * waves[0][k] for k in range(5)])
            for n in range(NVAR):
                part_ref[g, n * ROW + 2 * PARTS] = 6.0 * (
                    f_ref[d, i + 2, n] + f_ref[d, i + 3, n]
                ) + (df_ref[d, i + 1, n] - df_ref[d, i + 3, n])
                centre = du_ref[d, i + 2, n]
                part_ref[g, n * ROW + 2 * PARTS + 1] = (du_ref[d, i + 1, n] - centre) + (
                    du_ref[d, i + 3, n] - centre
                )
            return 0

        lax.fori_loop(first, last, step, 0)

    def advance(first, last):
        def step(g, _):
            alpha = alpha_ref[g]

            def wave(n):
                f = [part_ref[g, n * ROW + j] for j in range(PARTS)]
                t = [alpha * part_ref[g, n * ROW + PARTS + j] for j in range(PARTS)]
                rising = correction(f[0] + t[0], f[1] + t[1], f[3] + t[3], f[4] + t[4], f[5] + t[5])
                falling = correction(f[2] - t[2], f[1] - t[1], t[6] - f[6], t[5] - f[5], t[4] - f[4])
                return rising - falling

            def linear(n):
                at = n * ROW + 2 * PARTS
                return part_ref[g, at] + alpha * part_ref[g, at + 1]

            slower, faster = wave(NS), wave(NS + 3)
            shears = [wave(NS + 1), wave(NS + 2)]
            acoustic = slower + faster
            total, weighted = None, None
            for n in range(NS):
                amp = wave(n)
                flux_ref[g, n] = linear(n) + coef_ref[g, n] * acoustic + amp
                steep = coef_ref[g, STEEP + n] * amp
                total = amp if n == 0 else total + amp
                weighted = steep if n == 0 else weighted + steep
            amp = wave(NS + 4)
            flux_ref[g, NS + 4] = linear(NS + 4) + coef_ref[g, PASSIVE] * acoustic + amp
            mass = acoustic + total
            swing = coef_ref[g, GAMMA] * (faster - slower)
            vel = [coef_ref[g, VEL + n] for n in range(3)]
            flux_ref[g, NS] = linear(NS) + vel[0] * mass + swing
            flux_ref[g, NS + 1] = linear(NS + 1) + vel[1] * mass + shears[0]
            flux_ref[g, NS + 2] = linear(NS + 2) + vel[2] * mass + shears[1]
            flux_ref[g, NS + 3] = (
                linear(NS + 3)
                + coef_ref[g, SQUARE] * mass
                + (coef_ref[g, ENTHALPY] * acoustic - weighted)
                + vel[0] * swing
                + vel[1] * shears[0]
                + vel[2] * shears[1]
            )
            return 0

        lax.fori_loop(first, last, step, 0)

    for side, first in ((0, ny - 3), (1, 0)):
        for k in range(3):
            for r in range(NVAR):
                sy_ref[side, k, r] = turned(r, first + k)

    def x_state(x, best):
        u = [own(r, x) for r in range(NVAR)]
        inverse, vel, temp, pressure, gamma, sound = thermo(u, table_ref)
        for k, value in enumerate([inverse, *vel, temp, pressure, gamma, sound]):
            cache_ref[x, k] = value
        return tuple(jnp.maximum(b, jnp.abs(v) + sound) for b, v in zip(best, vel))

    zero = jnp.zeros(tile, jnp.float32)
    best = lax.fori_loop(0, 8, x_state, (zero, zero, zero))
    best = [jnp.max(b, axis=(0, 1), keepdims=True) for b in best]
    column = lax.broadcasted_iota(jnp.int32, (1, lanes), 1)
    mine_ref[...] = jnp.where(column == 0, best[0], jnp.where(column == 1, best[1], best[2]))
    pl.semaphore_wait(barrier, len(others))

    peers = []
    for n, (ox, oy) in enumerate(others):
        copy = pltpu.make_async_remote_copy(
            src_ref=mine_ref,
            dst_ref=slots_ref.at[n],
            send_sem=small_send.at[n],
            recv_sem=small_recv.at[n],
            device_id=there(ox, oy),
            device_id_type=MESH,
        )
        copy.start()
        peers.append(copy)
    halos = []
    for n, (origin, target, device) in enumerate(
        (
            (planes_ref.at[:, pl.ds(nx - 3, 3)], hx_ref.at[0], there(1, 0)),
            (planes_ref.at[:, pl.ds(0, 3)], hx_ref.at[1], there(size_x - 1, 0)),
            (sy_ref.at[0], hy_ref.at[0], there(0, 1)),
            (sy_ref.at[1], hy_ref.at[1], there(0, size_y - 1)),
        )
    ):
        copy = pltpu.make_async_remote_copy(
            src_ref=origin,
            dst_ref=target,
            send_sem=big_send.at[n],
            recv_sem=big_recv.at[n],
            device_id=device,
            device_id_type=MESH,
        )
        copy.start()
        halos.append(copy)

    def x_cells(x, _):
        u = [own(r, x) for r in range(NVAR)]
        state = [cache_ref[x, k] for k in range(8)]
        cells(0, x + 3, u, (state[0], state[1:4], *state[4:]))
        return 0

    side_by_side = lax.broadcasted_iota(jnp.int32, (block, lanes), 1) < block

    def flip(a):
        b = jnp.concatenate([a, a], axis=0).T
        return jnp.where(side_by_side, b[:block], b[block:])

    for r in range(NVAR):
        z_ref[pl.ds(r * block, block), :] = flip(x_ref[pl.ds(r * block, block), :])
    lax.fori_loop(0, 8, x_cells, 0)
    own_cells(1, turned)
    own_cells(2, upright)

    lane = lax.broadcasted_iota(jnp.int32, tile, 1)
    row = lax.broadcasted_iota(jnp.int32, tile, 0)
    walls = kind_ref[0] == 1, kind_ref[1] == 1
    outside = (row == 0) & (lane < block), (row == 7) & (lane >= block)
    wrap = row == 0, row == 7

    def beyond(side, r, k):
        inner = upright(r, (7 - k) if side else (2 - k))
        edge = upright(r, 7 if side else 0)
        ghost = jnp.where(walls[side], -inner if r == NS + 2 else inner, edge)
        if side:
            along = pltpu.roll(upright(r, k), 7, 0)
        else:
            along = pltpu.roll(upright(r, 5 + k), 1, 0)
        across = pltpu.roll(along, block, 1)
        return jnp.where(outside[side], ghost, jnp.where(wrap[side], across, along))

    halo_cells(2, beyond)
    differences(0, 3, 10)
    differences(1, 3, 10)
    differences(2, 0, 13)
    project(2, 0, 9, 0)
    project(1, 3, 6, 9)
    project(0, 3, 6, 12)

    for copy in peers:
        copy.wait()
    value = mine_ref[...]
    for n in range(len(others)):
        value = jnp.maximum(value, slots_ref[n])
    alphas = [
        jnp.broadcast_to(
            jnp.max(jnp.where(column == d, value, 0.0), axis=1, keepdims=True), tile
        )
        for d in range(3)
    ]
    for g in range(3 * FACES):
        alpha_ref[g] = alphas[2 if g < 9 else 1 if g < 12 or 15 <= g < 21 else 0]

    advance(0, 15)
    for d, read, pair, start in (
        (1, lambda side, r, k: hy_ref[side, k, r], halos[2:], 15),
        (0, lambda side, r, k: hx_ref[side, r, k], halos[:2], 21),
    ):
        for copy in pair:
            copy.wait()
        halo_cells(d, read)
        differences(d, 0, 3)
        differences(d, 10, 13)
        project(d, 0, 3, start)
        project(d, 6, 9, start + 3)
        advance(start, start + 6)

    def slot(d, i):
        if d == 2:
            return i
        if 3 <= i < 6:
            return (9 if d else 12) + i - 3
        return (15 if d else 21) + (i if i < 3 else i - 3)

    scale = (-COURANT / 6.0) / (alphas[0] + alphas[1] + alphas[2])

    def rate(d, i, r):
        n = NS + ORDER[d].index(r - NS) if NS <= r < NS + 3 else r
        return flux_ref[slot(d, i + 1), n] - flux_ref[slot(d, i), n]

    for r in range(NVAR):
        for i in range(8):
            acc_ref[pl.ds(r * block + i, 8, stride=8), :] = rate(1, i, r)
            back_ref[pl.ds(r * block + i, 8, stride=8), :] = rate(2, i, r)
        back = flip(back_ref[pl.ds(r * block, block), :])
        for i in range(8):
            rows = pl.ds(r * block + i * 8, 8)
            out_ref[rows, :] = scale * (
                rate(0, i, r) + acc_ref[rows, :] + back[i * 8 : i * 8 + 8]
            )


def shards(preserved_vector, nasa_table, gas_constant, species_index, face_kind):
    _, nx, ny, lanes = preserved_vector.shape
    size_x, size_y = lax.axis_size("gx"), lax.axis_size("gy")
    others = size_x * size_y - 1
    flat = preserved_vector.reshape(NVAR * nx * ny, lanes)
    hbm = pl.BlockSpec(memory_space=pltpu.HBM)
    dma = pltpu.SemaphoreType.DMA

    def buffer(*shape):
        return pltpu.VMEM(shape + (8, lanes), jnp.float32)

    out = pl.pallas_call(
        functools.partial(fused, size_x, size_y),
        out_shape=pltpu.VMEM(flat.shape, jnp.float32),
        in_specs=[hbm] * 6,
        out_specs=pl.BlockSpec(memory_space=pltpu.VMEM),
        scratch_shapes=[
            pltpu.SMEM(nasa_table.T.shape, jnp.float32),
            pltpu.SMEM(gas_constant.shape, jnp.float32),
            pltpu.SMEM(species_index.shape, jnp.int32),
            pltpu.SMEM((2,), jnp.int32),
            *[pltpu.VMEM(flat.shape, jnp.float32) for _ in range(4)],
            buffer(2, NVAR, 3),
            buffer(2, 3, NVAR),
            buffer(2, 3, NVAR),
            pltpu.VMEM((1, lanes), jnp.float32),
            pltpu.VMEM((others, 1, lanes), jnp.float32),
            buffer(TABLE),
            buffer(8, 8),
            buffer(3, 10, PRIMS),
            buffer(3, 14, NVAR + 1),
            buffer(3, 14, NVAR + 1),
            buffer(3, 13, NVAR + 1),
            buffer(3, 13, NVAR + 1),
            buffer(3 * FACES, NVAR * ROW),
            buffer(3 * FACES, COEFS),
            buffer(3 * FACES),
            buffer(3 * FACES, NVAR),
            dma(()),
            dma((4,)),
            dma((others,)),
            dma((others,)),
            dma((4,)),
            dma((4,)),
        ],
        compiler_params=pltpu.CompilerParams(
            collective_id=0, has_side_effects=True, vmem_limit_bytes=60 * 1000 * 1000
        ),
        name="increment",
    )(
        nasa_table.T, gas_constant, species_index, face_kind.reshape(2), flat,
        preserved_vector,
    )
    return out.reshape(preserved_vector.shape)


def solution(mesh):
    return jax.shard_map(
        shards,
        mesh=mesh,
        in_specs=(P(None, "gx", "gy", None), P(), P(), P(), P("gx", "gy", None)),
        out_specs=P(None, "gx", "gy", None),
        check_vma=False,
    )
```

```python
import functools

import jax
import jax.numpy as jnp
from jax import lax
from jax.experimental import pallas as pl
from jax.experimental.pallas import tpu as pltpu
from jax.sharding import PartitionSpec as P

NS = 9
NVAR = 14
EPSILON = 1e-06
COURANT = 0.8
TOTAL = NVAR
PRIMS = 24
VEL, PASSIVE, GAMMA, SOUND, SLOPES = 9, 12, 13, 14, 15
TABLE = 7 * NS
ORDER = ((0, 1, 2), (1, 0, 2), (2, 0, 1))
PARTS = 7
ROW = 2 * PARTS + 2
STEEP, ENTHALPY, SQUARE = 14, 23, 24
COEFS = 25
FACES = 9
MESH = pl.DeviceIdType.MESH


def fill_table(nasa_ref, gas_ref, index_ref, table_ref):
    for i in range(NS):
        row = index_ref[i]
        gas = gas_ref[row]
        values = [
            gas,
            gas * nasa_ref[5, row],
            gas * (nasa_ref[0, row] - 1.0),
            gas * nasa_ref[1, row] * (1.0 / 2.0),
            gas * nasa_ref[2, row] * (1.0 / 3.0),
            gas * nasa_ref[3, row] * (1.0 / 4.0),
            gas * nasa_ref[4, row] * (1.0 / 5.0),
        ]
        for n, value in enumerate(values):
            table_ref[n * NS + i] = jnp.full(table_ref.shape[1:], value, jnp.float32)


def tree(terms):
    terms = list(terms)
    while len(terms) > 1:
        terms = [a + b for a, b in zip(terms[::2], terms[1::2])] + (
            [terms[-1]] if len(terms) % 2 else []
        )
    return terms[0]


def thermo(u, table_ref):
    rho = tree(u[:NS])
    inverse = 1.0 / rho
    vel = [m * inverse for m in u[NS : NS + 3]]
    inner = u[NS + 3] - 0.5 * tree([v * m for v, m in zip(vel, u[NS : NS + 3])])
    mix = [tree([u[i] * table_ref[n * NS + i] for i in range(NS)]) for n in range(7)]
    gas, m6, m1, m2, m3, m4, m5 = mix
    c2, c3, c4, c5 = 2.0 * m2, 3.0 * m3, 4.0 * m4, 5.0 * m5
    temp = 1.0 - (tree([m6, m1, m2, m3, m4, m5]) - inner) / tree([m1, c2, c3, c4, c5])

    def heat(t):
        return m1 + t * (c2 + t * (c3 + t * (c4 + t * c5)))

    energy = m6 + temp * (m1 + temp * (m2 + temp * (m3 + temp * (m4 + temp * m5))))
    temp = temp - (energy - inner) / heat(temp)
    pressure = temp * gas
    gamma = gas / heat(temp)
    sound = jnp.sqrt((1.0 + gamma) * pressure * inverse)
    return inverse, vel, temp, pressure, gamma, sound


def slopes_of(temp, gamma, square, table_ref):
    kinetic = 0.5 * gamma * square
    result = []
    for i in range(NS):
        k = [table_ref[n * NS + i] for n in range(7)]
        e = k[1] + temp * (k[2] + temp * (k[3] + temp * (k[4] + temp * (k[5] + temp * k[6]))))
        result.append(k[0] * temp - gamma * e + kinetic)
    return result


def reciprocal(x):
    return pl.reciprocal(x, approx=True)


def correction(d1, d2, e0, e1, e2):
    h1, h2 = 0.75 * d1, 0.75 * d2
    near, far = h1 * d1 + 0.75 * EPSILON, h2 * d2 + 0.75 * EPSILON
    r0 = reciprocal(e0 * (e0 + h1) + near)
    r1 = reciprocal(e1 * (e1 + h1) + near)
    r2 = reciprocal(e2 * (e2 - h2) + far)
    a = r0 * r0 * (1.0 / 3.0)
    b = r1 * r1
    c = r2 * r2
    g0, g2 = e0 - e1, e1 - e2
    return (a * (g0 + g0) + c * g2) * reciprocal(a + c + (b + b))


def fused(
    size_x, size_y,
    nasa_hbm, gas_hbm, index_hbm, kind_hbm, flat_ref, planes_ref, out_ref,
    nasa_ref, gas_ref, index_ref, kind_ref,
    x_ref, z_ref, acc_ref, back_ref, hx_ref, sy_ref, hy_ref, mine_ref, slots_ref,
    table_ref, cache_ref, prim_ref, f_ref, u_ref, df_ref, du_ref,
    part_ref, coef_ref, alpha_ref, flux_ref, up_ref, down_ref,
    load_sem, param_sem, small_send, small_recv, big_send, big_recv,
):
    load = pltpu.make_async_copy(flat_ref, x_ref, load_sem)
    load.start()
    params = [
        pltpu.make_async_copy(origin, target, param_sem.at[n])
        for n, (origin, target) in enumerate(
            (
                (nasa_hbm, nasa_ref),
                (gas_hbm, gas_ref),
                (index_hbm, index_ref),
                (kind_hbm, kind_ref),
            )
        )
    ]
    for copy in params:
        copy.start()
    gx, gy = lax.axis_index("gx"), lax.axis_index("gy")
    nx, ny = planes_ref.shape[1], planes_ref.shape[2]
    lanes = x_ref.shape[1]
    tile = (8, lanes)
    block = nx * ny

    def there(ox, oy):
        return (lax.rem(gx + ox, size_x), lax.rem(gy + oy, size_y))

    others = [(ox, oy) for ox in range(size_x) for oy in range(size_y) if ox or oy]
    barrier = pltpu.get_barrier_semaphore()
    for ox, oy in others:
        pl.semaphore_signal(barrier, inc=1, device_id=there(ox, oy), device_id_type=MESH)
    for copy in params:
        copy.wait()
    fill_table(nasa_ref, gas_ref, index_ref, table_ref)
    load.wait()

    def own(r, x):
        return x_ref[pl.ds(pl.multiple_of(r * block + x * 8, 8), 8), :]

    def turned(r, y):
        return x_ref[pl.ds(r * block + y, 8, stride=8), :]

    def upright(r, t):
        return z_ref[pl.ds(r * block + t, 8, stride=8), :]

    def flow(d, p, u, vel, pressure):
        order = ORDER[d]
        speed = vel[order[0]]
        half, push = 0.5 * speed, 0.5 * pressure
        rows = list(range(NS)) + [NS + n for n in order] + [NS + 3, NS + 4]
        for k, r in enumerate(rows):
            value = u[r] * half
            if k == NS:
                value = value + push
            if k == NS + 3:
                value = value + push * speed
            f_ref[d, p, k] = value
            u_ref[d, p, k] = 0.5 * u[r]
        rho = tree(u[:NS])
        f_ref[d, p, TOTAL] = rho * half
        u_ref[d, p, TOTAL] = 0.5 * rho

    def cells(d, p, u, state):
        inverse, vel, temp, pressure, gamma, sound = state
        flow(d, p, u, vel, pressure)
        q = p - 2
        for k in range(NS):
            prim_ref[d, q, k] = u[k] * inverse
        for k in range(3):
            prim_ref[d, q, VEL + k] = vel[ORDER[d][k]]
        prim_ref[d, q, PASSIVE] = u[NS + 4] * inverse
        prim_ref[d, q, GAMMA] = gamma
        prim_ref[d, q, SOUND] = sound
        square = tree([v * v for v in vel])
        for k, value in enumerate(slopes_of(temp, gamma, square, table_ref)):
            prim_ref[d, q, SLOPES + k] = value

    def own_cells(d, read):
        def step(n, _):
            u = [read(r, n) for r in range(NVAR)]
            cells(d, n + 3, u, thermo(u, table_ref))
            return 0

        lax.fori_loop(0, 8, step, 0, unroll=2)

    def halo_cells(d, side, read):
        for k in range(3):
            p = k + 11 * side
            u = [read(side, r, k) for r in range(NVAR)]
            state = thermo(u, table_ref)
            if p in (2, 11):
                cells(d, p, u, state)
            else:
                flow(d, p, u, state[1], state[3])

    def differences(d, first, last):
        def step(p, _):
            for k in range(NVAR + 1):
                df_ref[d, p, k] = f_ref[d, p + 1, k] - f_ref[d, p, k]
                du_ref[d, p, k] = u_ref[d, p + 1, k] - u_ref[d, p, k]
            return 0

        lax.fori_loop(first, last, step, 0)

    def split_inner(d):
        def step(p, _):
            for k in range(NVAR + 1):
                push = alphas[d] * du_ref[d, p, k]
                up_ref[d, p, k] = df_ref[d, p, k] + push
                down_ref[d, p, k] = df_ref[d, p, k] - push
            return 0

        lax.fori_loop(3, 10, step, 0)

    def split_outer(d, first):
        def step(p, _):
            for k in range(NVAR + 1):
                step_f = f_ref[d, p + 1, k] - f_ref[d, p, k]
                push = alphas[d] * (u_ref[d, p + 1, k] - u_ref[d, p, k])
                up_ref[d, p, k] = step_f + push
                down_ref[d, p, k] = step_f - push
            return 0

        lax.fori_loop(first, first + 3, step, 0)

    def means(d, i):
        def mean(q):
            return 0.5 * (prim_ref[d, i, q] + prim_ref[d, i + 1, q])

        y = [mean(k) for k in range(NS)]
        vel = [mean(VEL + k) for k in range(3)]
        phi = [mean(SLOPES + k) for k in range(NS)]
        return y, vel, phi, mean(PASSIVE), mean(GAMMA), mean(SOUND)

    def waves_of(get, vel, phi, gamma, inv2, half_inv):
        s = get(TOTAL)
        m = [get(NS + n) for n in range(3)]
        dp = tree([phi[n] * get(n) for n in range(NS)]) + gamma * (
            get(NS + 3) - tree([vel[n] * m[n] for n in range(3)])
        )
        scaled = dp * inv2
        jump = (m[0] - vel[0] * s) * half_inv
        middle = 0.5 * scaled
        return scaled, middle - jump, m[1] - vel[1] * s, m[2] - vel[2] * s, middle + jump

    def project(d, first, last, start):
        def step(i, _):
            g = i + (start - first)
            y, vel, phi, z, gamma, sound = means(d, i)
            inv = 1.0 / sound
            inv2, half_inv = inv * inv, 0.5 * inv
            steep = 1.0 / gamma
            for k in range(NS):
                coef_ref[g, k] = y[k]
                coef_ref[g, STEEP + k] = phi[k] * steep
            for k in range(3):
                coef_ref[g, VEL + k] = vel[k]
            coef_ref[g, PASSIVE] = z
            coef_ref[g, GAMMA] = sound
            coef_ref[g, ENTHALPY] = (
                sound * sound - tree([a * b for a, b in zip(y, phi)])
            ) * steep
            coef_ref[g, SQUARE] = tree([v * v for v in vel])
            for half, ref in enumerate((df_ref, du_ref)):

                def keep(n, d5):
                    at = n * ROW + half * PARTS
                    for j in range(3):
                        part_ref[g, at + j] = d5[j + 1]
                    for j in range(4):
                        part_ref[g, at + 3 + j] = d5[j + 1] - d5[j]

                waves = [
                    waves_of(lambda n: ref[d, i + k, n], vel, phi, gamma, inv2, half_inv)
                    for k in range(5)
                ]
                for n in range(4):
                    keep(NS + n, [w[n + 1] for w in waves])
                for n, share in enumerate(y):
                    keep(n, [ref[d, i + k, n] - share * waves[k][0] for k in range(5)])
                keep(NS + 4, [ref[d, i + k, NS + 4] - z * waves[k][0] for k in range(5)])
            for n in range(NVAR):
                part_ref[g, n * ROW + 2 * PARTS] = 6.0 * (
                    f_ref[d, i + 2, n] + f_ref[d, i + 3, n]
                ) + (df_ref[d, i + 1, n] - df_ref[d, i + 3, n])
                centre = du_ref[d, i + 2, n]
                part_ref[g, n * ROW + 2 * PARTS + 1] = (du_ref[d, i + 1, n] - centre) + (
                    du_ref[d, i + 3, n] - centre
                )
            return 0

        lax.fori_loop(first, last, step, 0)

    def advance(first, last):
        def step(g, _):
            alpha = alpha_ref[g]

            def wave(n):
                f = [part_ref[g, n * ROW + j] for j in range(PARTS)]
                t = [alpha * part_ref[g, n * ROW + PARTS + j] for j in range(PARTS)]
                rising = correction(f[0] + t[0], f[1] + t[1], f[3] + t[3], f[4] + t[4], f[5] + t[5])
                falling = correction(f[2] - t[2], f[1] - t[1], t[6] - f[6], t[5] - f[5], t[4] - f[4])
                return rising - falling

            def linear(n):
                at = n * ROW + 2 * PARTS
                return part_ref[g, at] + alpha * part_ref[g, at + 1]

            slower, faster = wave(NS), wave(NS + 3)
            shears = [wave(NS + 1), wave(NS + 2)]
            acoustic = slower + faster
            total, weighted = None, None
            for n in range(NS):
                amp = wave(n)
                flux_ref[g, n] = linear(n) + coef_ref[g, n] * acoustic + amp
                steep = coef_ref[g, STEEP + n] * amp
                total = amp if n == 0 else total + amp
                weighted = steep if n == 0 else weighted + steep
            amp = wave(NS + 4)
            flux_ref[g, NS + 4] = linear(NS + 4) + coef_ref[g, PASSIVE] * acoustic + amp
            mass = acoustic + total
            swing = coef_ref[g, GAMMA] * (faster - slower)
            vel = [coef_ref[g, VEL + n] for n in range(3)]
            flux_ref[g, NS] = linear(NS) + vel[0] * mass + swing
            flux_ref[g, NS + 1] = linear(NS + 1) + vel[1] * mass + shears[0]
            flux_ref[g, NS + 2] = linear(NS + 2) + vel[2] * mass + shears[1]
            flux_ref[g, NS + 3] = (
                linear(NS + 3)
                + coef_ref[g, SQUARE] * mass
                + (coef_ref[g, ENTHALPY] * acoustic - weighted)
                + vel[0] * swing
                + vel[1] * shears[0]
                + vel[2] * shears[1]
            )
            return 0

        lax.fori_loop(first, last, step, 0)

    side_by_side = lax.broadcasted_iota(jnp.int32, (block, lanes), 1) < block

    def flip(a):
        b = jnp.concatenate([a, a], axis=0).T
        return jnp.where(side_by_side, b[:block], b[block:])

    def turn_back(r):
        rows = pl.ds(pl.multiple_of(r * block, block), block)
        back_ref[rows, :] = flip(back_ref[rows, :])

    def direct(d, first, last, start):
        def step(i, _):
            g = i + (start - first)
            y, vel, phi, z, gamma, sound = means(d, i)
            inv = 1.0 / sound
            inv2, half_inv = inv * inv, 0.5 * inv

            def rising(n, k):
                return up_ref[d, i + k, n]

            def falling(n, k):
                return down_ref[d, i + 4 - k, n]

            sides = [
                [
                    waves_of(lambda n: get(n, k), vel, phi, gamma, inv2, half_inv)
                    for k in range(4)
                ]
                for get in (rising, falling)
            ]

            def both(up, down):
                pair = [
                    correction(v[1], v[2], v[1] - v[0], v[2] - v[1], v[3] - v[2])
                    for v in (up, down)
                ]
                return pair[0] - pair[1]

            def wave(n):
                return both(*[[w[n] for w in side] for side in sides])

            def carried(n, share):
                return both(
                    [rising(n, k) - share * sides[0][k][0] for k in range(4)],
                    [falling(n, k) - share * sides[1][k][0] for k in range(4)],
                )

            def linear(n):
                ahead = up_ref[d, i + 2, n] - down_ref[d, i + 2, n]
                return 6.0 * (f_ref[d, i + 2, n] + f_ref[d, i + 3, n]) + (
                    (up_ref[d, i + 1, n] - down_ref[d, i + 3, n]) - ahead
                )

            slower, faster = wave(1), wave(4)
            shears = [wave(2), wave(3)]
            acoustic = slower + faster
            total, weighted = None, None
            for n in range(NS):
                amp = carried(n, y[n])
                flux_ref[g, n] = linear(n) + y[n] * acoustic + amp
                term = phi[n] * amp
                total = amp if n == 0 else total + amp
                weighted = term if n == 0 else weighted + term
            amp = carried(NS + 4, z)
            flux_ref[g, NS + 4] = linear(NS + 4) + z * acoustic + amp
            mass = acoustic + total
            swing = sound * (faster - slower)
            flux_ref[g, NS] = linear(NS) + vel[0] * mass + swing
            flux_ref[g, NS + 1] = linear(NS + 1) + vel[1] * mass + shears[0]
            flux_ref[g, NS + 2] = linear(NS + 2) + vel[2] * mass + shears[1]
            blend = tree([a * b for a, b in zip(y, phi)])
            flux_ref[g, NS + 3] = (
                linear(NS + 3)
                + tree([v * v for v in vel]) * mass
                + ((sound * sound - blend) * acoustic - weighted) / gamma
                + vel[0] * swing
                + vel[1] * shears[0]
                + vel[2] * shears[1]
            )
            turn_back(g - 15)
            return 0

        lax.fori_loop(first, last, step, 0)

    for side, first in ((0, ny - 3), (1, 0)):
        for k in range(3):
            for r in range(NVAR):
                sy_ref[side, k, r] = turned(r, first + k)

    def x_state(x, best):
        u = [own(r, x) for r in range(NVAR)]
        inverse, vel, temp, pressure, gamma, sound = thermo(u, table_ref)
        for k, value in enumerate([inverse, *vel, temp, pressure, gamma, sound]):
            cache_ref[x, k] = value
        return tuple(jnp.maximum(b, jnp.abs(v) + sound) for b, v in zip(best, vel))

    zero = jnp.zeros(tile, jnp.float32)
    best = lax.fori_loop(0, 8, x_state, (zero, zero, zero), unroll=2)
    best = [jnp.max(b, axis=(0, 1), keepdims=True) for b in best]
    column = lax.broadcasted_iota(jnp.int32, (1, lanes), 1)
    mine_ref[...] = jnp.where(column == 0, best[0], jnp.where(column == 1, best[1], best[2]))
    def x_cells(x, _):
        u = [own(r, x) for r in range(NVAR)]
        state = [cache_ref[x, k] for k in range(8)]
        cells(0, x + 3, u, (state[0], state[1:4], *state[4:]))
        return 0

    for r in range(NVAR):
        z_ref[pl.ds(r * block, block), :] = flip(x_ref[pl.ds(r * block, block), :])
    lax.fori_loop(0, 8, x_cells, 0)
    own_cells(1, turned)
    pl.semaphore_wait(barrier, len(others))

    for n, (ox, oy) in enumerate(others):
        copy = pltpu.make_async_remote_copy(
            src_ref=mine_ref,
            dst_ref=slots_ref.at[n],
            send_sem=small_send,
            recv_sem=small_recv,
            device_id=there(ox, oy),
            device_id_type=MESH,
        )
        copy.start()
    own_cells(2, upright)

    lane = lax.broadcasted_iota(jnp.int32, tile, 1)
    row = lax.broadcasted_iota(jnp.int32, tile, 0)
    walls = kind_ref[0] == 1, kind_ref[1] == 1
    outside = (row == 0) & (lane < block), (row == 7) & (lane >= block)
    wrap = row == 0, row == 7

    def beyond(side, r, k):
        inner = upright(r, (7 - k) if side else (2 - k))
        edge = upright(r, 7 if side else 0)
        ghost = jnp.where(walls[side], -inner if r == NS + 2 else inner, edge)
        if side:
            along = pltpu.roll(upright(r, k), 7, 0)
        else:
            along = pltpu.roll(upright(r, 5 + k), 1, 0)
        across = pltpu.roll(along, block, 1)
        return jnp.where(outside[side], ghost, jnp.where(wrap[side], across, along))

    halos = []
    for n, (origin, target, device) in enumerate(
        (
            (planes_ref.at[:, pl.ds(nx - 3, 3)], hx_ref.at[0], there(1, 0)),
            (planes_ref.at[:, pl.ds(0, 3)], hx_ref.at[1], there(size_x - 1, 0)),
            (sy_ref.at[0], hy_ref.at[0], there(0, 1)),
            (sy_ref.at[1], hy_ref.at[1], there(0, size_y - 1)),
        )
    ):
        copy = pltpu.make_async_remote_copy(
            src_ref=origin,
            dst_ref=target,
            send_sem=big_send.at[n],
            recv_sem=big_recv.at[n],
            device_id=device,
            device_id_type=MESH,
        )
        copy.start()
        halos.append(copy)

    for side in range(2):
        halo_cells(2, side, beyond)
    differences(0, 3, 10)
    differences(1, 3, 10)
    differences(2, 0, 13)
    project(2, 0, 9, 0)
    project(1, 3, 6, 9)
    project(0, 3, 6, 12)

    for sem in (small_recv, small_send):
        pltpu.make_async_copy(slots_ref, slots_ref, sem).wait()
    value = mine_ref[...]
    for n in range(len(others)):
        value = jnp.maximum(value, slots_ref[n])
    alphas = [
        jnp.broadcast_to(
            jnp.max(jnp.where(column == d, value, 0.0), axis=1, keepdims=True), tile
        )
        for d in range(3)
    ]
    for g in range(15):
        alpha_ref[g] = alphas[2 if g < 9 else 1 if g < 12 else 0]
    scale = (-COURANT / 6.0) / (alphas[0] + alphas[1] + alphas[2])

    def slot(d, i):
        if d == 2:
            return i
        if 3 <= i < 6:
            return (9 if d else 12) + i - 3
        return (15 if d else 21) + (i if i < 3 else i - 3)

    def rate(d, i, r):
        n = NS + ORDER[d].index(r - NS) if NS <= r < NS + 3 else r
        return flux_ref[slot(d, i + 1), n] - flux_ref[slot(d, i), n]

    advance(0, 15)
    for r in range(NVAR):
        for i in range(8):
            back_ref[pl.ds(r * block + i, 8, stride=8), :] = rate(2, i, r)
    for d, read, pair, start in (
        (1, lambda side, r, k: hy_ref[side, k, r], halos[2:], 15),
        (0, lambda side, r, k: hx_ref[side, r, k], halos[:2], 21),
    ):
        split_inner(d)
        for side, copy in enumerate(pair):
            copy.wait()
            halo_cells(d, side, read)
            split_outer(d, 10 * side)
            direct(d, 6 * side, 6 * side + 3, start + 3 * side)
    for r in range(12, NVAR):
        turn_back(r)
    for r in range(NVAR):
        for i in range(8):
            acc_ref[pl.ds(r * block + i, 8, stride=8), :] = rate(1, i, r)
    for r in range(NVAR):
        for i in range(8):
            rows = pl.ds(r * block + i * 8, 8)
            out_ref[rows, :] = scale * (rate(0, i, r) + acc_ref[rows, :] + back_ref[rows, :])


def shards(preserved_vector, nasa_table, gas_constant, species_index, face_kind):
    _, nx, ny, lanes = preserved_vector.shape
    size_x, size_y = lax.axis_size("gx"), lax.axis_size("gy")
    others = size_x * size_y - 1
    flat = preserved_vector.reshape(NVAR * nx * ny, lanes)
    hbm = pl.BlockSpec(memory_space=pltpu.HBM)
    dma = pltpu.SemaphoreType.DMA

    def buffer(*shape):
        return pltpu.VMEM(shape + (8, lanes), jnp.float32)

    out = pl.pallas_call(
        functools.partial(fused, size_x, size_y),
        out_shape=pltpu.VMEM(flat.shape, jnp.float32),
        in_specs=[hbm] * 6,
        out_specs=pl.BlockSpec(memory_space=pltpu.VMEM),
        scratch_shapes=[
            pltpu.SMEM(nasa_table.T.shape, jnp.float32),
            pltpu.SMEM(gas_constant.shape, jnp.float32),
            pltpu.SMEM(species_index.shape, jnp.int32),
            pltpu.SMEM((2,), jnp.int32),
            *[pltpu.VMEM(flat.shape, jnp.float32) for _ in range(4)],
            buffer(2, NVAR, 3),
            buffer(2, 3, NVAR),
            buffer(2, 3, NVAR),
            pltpu.VMEM((1, lanes), jnp.float32),
            pltpu.VMEM((others, 1, lanes), jnp.float32),
            buffer(TABLE),
            buffer(8, 8),
            buffer(3, 10, PRIMS),
            buffer(3, 14, NVAR + 1),
            buffer(3, 14, NVAR + 1),
            buffer(3, 13, NVAR + 1),
            buffer(3, 13, NVAR + 1),
            buffer(15, NVAR * ROW),
            buffer(15, COEFS),
            buffer(15),
            buffer(3 * FACES, NVAR),
            buffer(2, 13, NVAR + 1),
            buffer(2, 13, NVAR + 1),
            dma(()),
            dma((4,)),
            dma(()),
            dma(()),
            dma((4,)),
            dma((4,)),
        ],
        compiler_params=pltpu.CompilerParams(
            collective_id=0, has_side_effects=True, vmem_limit_bytes=60 * 1000 * 1000
        ),
        name="increment",
    )(
        nasa_table.T, gas_constant, species_index, face_kind.reshape(2), flat,
        preserved_vector,
    )
    return out.reshape(preserved_vector.shape)


def solution(mesh):
    return jax.shard_map(
        shards,
        mesh=mesh,
        in_specs=(P(None, "gx", "gy", None), P(), P(), P(), P("gx", "gy", None)),
        out_specs=P(None, "gx", "gy", None),
        check_vma=False,
    )
```

```python
import functools

import jax
import jax.numpy as jnp
from jax import lax
from jax.experimental import pallas as pl
from jax.experimental.pallas import tpu as pltpu
from jax.sharding import PartitionSpec as P

NS = 9
NVAR = 14
EPSILON = 1e-06
COURANT = 0.8
TOTAL = NVAR
PRIMS = 24
VEL, PASSIVE, GAMMA, SOUND, SLOPES = 9, 12, 13, 14, 15
TABLE = 7 * NS
ORDER = ((0, 1, 2), (1, 0, 2), (2, 0, 1))
PARTS = 7
ROW = 2 * PARTS + 2
STEEP, ENTHALPY, SQUARE = 14, 23, 24
COEFS = 25
FACES = 9
MESH = pl.DeviceIdType.MESH


def fill_table(nasa_ref, gas_ref, index_ref, table_ref):
    for i in range(NS):
        row = index_ref[i]
        gas = gas_ref[row]
        values = [
            gas,
            gas * nasa_ref[5, row],
            gas * (nasa_ref[0, row] - 1.0),
            gas * nasa_ref[1, row] * (1.0 / 2.0),
            gas * nasa_ref[2, row] * (1.0 / 3.0),
            gas * nasa_ref[3, row] * (1.0 / 4.0),
            gas * nasa_ref[4, row] * (1.0 / 5.0),
        ]
        for n, value in enumerate(values):
            table_ref[n * NS + i] = jnp.full(table_ref.shape[1:], value, jnp.float32)


def tree(terms):
    terms = list(terms)
    while len(terms) > 1:
        terms = [a + b for a, b in zip(terms[::2], terms[1::2])] + (
            [terms[-1]] if len(terms) % 2 else []
        )
    return terms[0]


def thermo(u, table_ref):
    rho = tree(u[:NS])
    inverse = 1.0 / rho
    vel = [m * inverse for m in u[NS : NS + 3]]
    inner = u[NS + 3] - 0.5 * tree([v * m for v, m in zip(vel, u[NS : NS + 3])])
    mix = [tree([u[i] * table_ref[n * NS + i] for i in range(NS)]) for n in range(7)]
    gas, m6, m1, m2, m3, m4, m5 = mix
    c2, c3, c4, c5 = 2.0 * m2, 3.0 * m3, 4.0 * m4, 5.0 * m5
    temp = 1.0 - (tree([m6, m1, m2, m3, m4, m5]) - inner) / tree([m1, c2, c3, c4, c5])

    def heat(t):
        return m1 + t * (c2 + t * (c3 + t * (c4 + t * c5)))

    energy = m6 + temp * (m1 + temp * (m2 + temp * (m3 + temp * (m4 + temp * m5))))
    temp = temp - (energy - inner) / heat(temp)
    pressure = temp * gas
    gamma = gas / heat(temp)
    sound = jnp.sqrt((1.0 + gamma) * pressure * inverse)
    return inverse, vel, temp, pressure, gamma, sound


def half_slopes(temp, gamma, vel, table_ref):
    warm, lean = 0.5 * temp, 0.5 * gamma
    kinetic = (0.5 * lean) * tree([v * v for v in vel])
    result = []
    for i in range(NS):
        k = [table_ref[n * NS + i] for n in range(7)]
        e = k[1] + temp * (k[2] + temp * (k[3] + temp * (k[4] + temp * (k[5] + temp * k[6]))))
        result.append(k[0] * warm - lean * e + kinetic)
    return result


def reciprocal(x):
    return pl.reciprocal(x, approx=True)


def correction(d1, d2, e0, e1, e2):
    h1, h2 = 0.75 * d1, 0.75 * d2
    near, far = h1 * d1 + 0.75 * EPSILON, h2 * d2 + 0.75 * EPSILON
    r0 = reciprocal(e0 * (e0 + h1) + near)
    r1 = reciprocal(e1 * (e1 + h1) + near)
    r2 = reciprocal(e2 * (e2 - h2) + far)
    a = r0 * r0 * (1.0 / 3.0)
    b = r1 * r1
    c = r2 * r2
    g0, g2 = e0 - e1, e1 - e2
    return (a * (g0 + g0) + c * g2) * reciprocal(a + c + (b + b))


def fused(
    size_x, size_y,
    nasa_hbm, gas_hbm, index_hbm, kind_hbm, flat_ref, planes_ref, out_ref,
    nasa_ref, gas_ref, index_ref, kind_ref,
    x_ref, z_ref, acc_ref, back_ref, hx_ref, sy_ref, hy_ref, mine_ref, slots_ref,
    table_ref, cache_ref, prim_ref, f_ref, u_ref, df_ref, du_ref,
    part_ref, coef_ref, flux_ref, up_ref, down_ref,
    load_sem, param_sem, small_send, small_recv, big_send, big_recv,
):
    load = pltpu.make_async_copy(flat_ref, x_ref, load_sem)
    load.start()
    params = [
        pltpu.make_async_copy(origin, target, param_sem.at[n])
        for n, (origin, target) in enumerate(
            (
                (nasa_hbm, nasa_ref),
                (gas_hbm, gas_ref),
                (index_hbm, index_ref),
                (kind_hbm, kind_ref),
            )
        )
    ]
    for copy in params:
        copy.start()
    gx, gy = lax.axis_index("gx"), lax.axis_index("gy")
    nx, ny = planes_ref.shape[1], planes_ref.shape[2]
    lanes = x_ref.shape[1]
    tile = (8, lanes)
    block = nx * ny

    def there(ox, oy):
        return (lax.rem(gx + ox, size_x), lax.rem(gy + oy, size_y))

    others = [(ox, oy) for ox in range(size_x) for oy in range(size_y) if ox or oy]
    barrier = pltpu.get_barrier_semaphore()
    for ox, oy in others:
        pl.semaphore_signal(barrier, inc=1, device_id=there(ox, oy), device_id_type=MESH)
    for copy in params:
        copy.wait()
    fill_table(nasa_ref, gas_ref, index_ref, table_ref)
    load.wait()

    def own(r, x):
        return x_ref[pl.ds(pl.multiple_of(r * block + x * 8, 8), 8), :]

    def turned(r, y):
        return x_ref[pl.ds(r * block + y, 8, stride=8), :]

    def upright(r, t):
        return z_ref[pl.ds(r * block + t, 8, stride=8), :]

    def flow(d, p, u, vel, pressure):
        order = ORDER[d]
        speed = vel[order[0]]
        half, push = 0.5 * speed, 0.5 * pressure
        rows = list(range(NS)) + [NS + n for n in order] + [NS + 3, NS + 4]
        for k, r in enumerate(rows):
            value = u[r] * half
            if k == NS:
                value = value + push
            if k == NS + 3:
                value = value + push * speed
            f_ref[d, p, k] = value
            u_ref[d, p, k] = 0.5 * u[r]
        rho = tree(u[:NS])
        f_ref[d, p, TOTAL] = rho * half
        u_ref[d, p, TOTAL] = 0.5 * rho

    def cells(d, p, u, state):
        inverse, vel, temp, pressure, gamma, sound = state
        flow(d, p, u, vel, pressure)
        q = p - 2
        share = 0.5 * inverse
        for k in range(NS):
            prim_ref[d, q, k] = u[k] * share
        for k in range(3):
            prim_ref[d, q, VEL + k] = 0.5 * vel[ORDER[d][k]]
        prim_ref[d, q, PASSIVE] = u[NS + 4] * share
        prim_ref[d, q, GAMMA] = 0.5 * gamma
        prim_ref[d, q, SOUND] = 0.5 * sound
        for k, value in enumerate(half_slopes(temp, gamma, vel, table_ref)):
            prim_ref[d, q, SLOPES + k] = value

    def own_cells(d, read):
        def step(n, _):
            u = [read(r, n) for r in range(NVAR)]
            cells(d, n + 3, u, thermo(u, table_ref))
            return 0

        lax.fori_loop(0, 8, step, 0, unroll=2)

    def halo_cells(d, side, read):
        for k in range(3):
            p = k + 11 * side
            u = [read(side, r, k) for r in range(NVAR)]
            state = thermo(u, table_ref)
            if p in (2, 11):
                cells(d, p, u, state)
            else:
                flow(d, p, u, state[1], state[3])

    def differences(d, first, last):
        def step(p, _):
            for k in range(NVAR + 1):
                df_ref[d, p, k] = f_ref[d, p + 1, k] - f_ref[d, p, k]
                du_ref[d, p, k] = u_ref[d, p + 1, k] - u_ref[d, p, k]
            return 0

        lax.fori_loop(first, last, step, 0)

    def split_inner(d):
        def step(p, _):
            for k in range(NVAR + 1):
                push = alphas[d] * du_ref[d, p, k]
                up_ref[d, p, k] = df_ref[d, p, k] + push
                down_ref[d, p, k] = df_ref[d, p, k] - push
            return 0

        lax.fori_loop(3, 10, step, 0)

    def split_outer(d, first):
        def step(p, _):
            for k in range(NVAR + 1):
                step_f = f_ref[d, p + 1, k] - f_ref[d, p, k]
                push = alphas[d] * (u_ref[d, p + 1, k] - u_ref[d, p, k])
                up_ref[d, p, k] = step_f + push
                down_ref[d, p, k] = step_f - push
            return 0

        lax.fori_loop(first, first + 3, step, 0)

    def means(d, i):
        def mean(q):
            return prim_ref[d, i, q] + prim_ref[d, i + 1, q]

        y = [mean(k) for k in range(NS)]
        vel = [mean(VEL + k) for k in range(3)]
        phi = [mean(SLOPES + k) for k in range(NS)]
        return y, vel, phi, mean(PASSIVE), mean(GAMMA), mean(SOUND)

    def keep_means(d, i, g):
        y, vel, phi, z, gamma, sound = means(d, i)
        inv = 1.0 / sound
        steep = 1.0 / gamma
        for k in range(NS):
            coef_ref[g, k] = y[k]
            coef_ref[g, STEEP + k] = phi[k] * steep
        for k in range(3):
            coef_ref[g, VEL + k] = vel[k]
        coef_ref[g, PASSIVE] = z
        coef_ref[g, GAMMA] = sound
        coef_ref[g, ENTHALPY] = (sound * sound - tree([a * b for a, b in zip(y, phi)])) * steep
        coef_ref[g, SQUARE] = tree([v * v for v in vel])
        return y, vel, phi, z, gamma, inv * inv, 0.5 * inv

    def waves_of(get, vel, phi, gamma, inv2, half_inv):
        s = get(TOTAL)
        m = [get(NS + n) for n in range(3)]
        dp = tree([phi[n] * get(n) for n in range(NS)]) + gamma * (
            get(NS + 3) - tree([vel[n] * m[n] for n in range(3)])
        )
        scaled = dp * inv2
        jump = (m[0] - vel[0] * s) * half_inv
        middle = 0.5 * scaled
        return scaled, middle - jump, m[1] - vel[1] * s, m[2] - vel[2] * s, middle + jump

    def project(d, first, last, start):
        def step(i, _):
            g = i + (start - first)
            y, vel, phi, z, gamma, inv2, half_inv = keep_means(d, i, g)
            for half, ref in enumerate((df_ref, du_ref)):

                def keep(n, d5):
                    at = n * ROW + half * PARTS
                    for j in range(3):
                        part_ref[g, at + j] = d5[j + 1]
                    for j in range(4):
                        part_ref[g, at + 3 + j] = d5[j + 1] - d5[j]

                waves = [
                    waves_of(lambda n: ref[d, i + k, n], vel, phi, gamma, inv2, half_inv)
                    for k in range(5)
                ]
                for n in range(4):
                    keep(NS + n, [w[n + 1] for w in waves])
                for n, share in enumerate(y):
                    keep(n, [ref[d, i + k, n] - share * waves[k][0] for k in range(5)])
                keep(NS + 4, [ref[d, i + k, NS + 4] - z * waves[k][0] for k in range(5)])
            for n in range(NVAR):
                part_ref[g, n * ROW + 2 * PARTS] = 6.0 * (
                    f_ref[d, i + 2, n] + f_ref[d, i + 3, n]
                ) + (df_ref[d, i + 1, n] - df_ref[d, i + 3, n])
                centre = du_ref[d, i + 2, n]
                part_ref[g, n * ROW + 2 * PARTS + 1] = (du_ref[d, i + 1, n] - centre) + (
                    du_ref[d, i + 3, n] - centre
                )
            return 0

        lax.fori_loop(first, last, step, 0)

    def combine(d, g, c, wave, linear):
        slower, faster = wave(NS), wave(NS + 3)
        shears = [wave(NS + 1), wave(NS + 2)]
        acoustic = slower + faster
        total, weighted = None, None
        for n in range(NS):
            amp = wave(n)
            flux_ref[g, n] = linear(n) + coef_ref[c, n] * acoustic + amp
            steep = coef_ref[c, STEEP + n] * amp
            total = amp if n == 0 else total + amp
            weighted = steep if n == 0 else weighted + steep
        amp = wave(NS + 4)
        flux_ref[g, NS + 4] = linear(NS + 4) + coef_ref[c, PASSIVE] * acoustic + amp
        mass = acoustic + total
        swing = coef_ref[c, GAMMA] * (faster - slower)
        vel = [coef_ref[c, VEL + n] for n in range(3)]
        moved = [swing] + shears
        for n, r in enumerate(ORDER[d]):
            flux_ref[g, NS + r] = linear(NS + n) + vel[n] * mass + moved[n]
        flux_ref[g, NS + 3] = (
            linear(NS + 3)
            + coef_ref[c, SQUARE] * mass
            + (coef_ref[c, ENTHALPY] * acoustic - weighted)
            + tree([v * m for v, m in zip(vel, moved)])
        )

    def advance(d, first, last):
        def step(g, _):
            alpha = alphas[d]

            def wave(n):
                f = [part_ref[g, n * ROW + j] for j in range(PARTS)]
                t = [alpha * part_ref[g, n * ROW + PARTS + j] for j in range(PARTS)]
                rising = correction(f[0] + t[0], f[1] + t[1], f[3] + t[3], f[4] + t[4], f[5] + t[5])
                falling = correction(f[2] - t[2], f[1] - t[1], t[6] - f[6], t[5] - f[5], t[4] - f[4])
                return rising - falling

            def linear(n):
                at = n * ROW + 2 * PARTS
                return part_ref[g, at] + alpha * part_ref[g, at + 1]

            combine(d, g, g, wave, linear)
            return 0

        lax.fori_loop(first, last, step, 0)

    side_by_side = lax.broadcasted_iota(jnp.int32, (block, lanes), 1) < block

    def flip(a):
        b = jnp.concatenate([a, a], axis=0).T
        return jnp.where(side_by_side, b[:block], b[block:])

    def turn_back(r):
        rows = pl.ds(pl.multiple_of(r * block, block), block)
        z_ref[rows, :] = flip(back_ref[rows, :])

    def slot(d, i):
        if d == 2:
            return i
        if 3 <= i < 6:
            return (9 if d else 12) + i - 3
        return (15 if d else 21) + (i if i < 3 else i - 3)

    def rate(d, i, r):
        return flux_ref[slot(d, i + 1), r] - flux_ref[slot(d, i), r]

    def gather_y(r):
        for i in range(8):
            acc_ref[pl.ds(r * block + i, 8, stride=8), :] = rate(1, i, r)

    def outer_face(h):
        return jnp.where(h < 3, h, h + 3)

    def lay(d, first, last):
        def step(h, _):
            i = outer_face(h)
            y, vel, phi, z, gamma, inv2, half_inv = keep_means(d, i, h)
            for side, get in enumerate(
                (
                    lambda n, k: up_ref[d, i + k, n],
                    lambda n, k: down_ref[d, i + 4 - k, n],
                )
            ):
                for k in range(4):
                    at = 4 * side + k
                    waves = waves_of(lambda n: get(n, k), vel, phi, gamma, inv2, half_inv)
                    for n in range(4):
                        part_ref[h, (NS + n) * 8 + at] = waves[n + 1]
                    for n in range(NS):
                        part_ref[h, n * 8 + at] = get(n, k) - y[n] * waves[0]
                    part_ref[h, (NS + 4) * 8 + at] = get(NS + 4, k) - z * waves[0]
            return 0

        lax.fori_loop(first, last, step, 0)

    def close(d, first, last):
        def step(h, _):
            i = outer_face(h)

            def wave(n):
                pair = []
                for side in range(2):
                    v = [part_ref[h, n * 8 + side * 4 + k] for k in range(4)]
                    pair.append(correction(v[1], v[2], v[1] - v[0], v[2] - v[1], v[3] - v[2]))
                return pair[0] - pair[1]

            def linear(n):
                ahead = up_ref[d, i + 2, n] - down_ref[d, i + 2, n]
                return 6.0 * (f_ref[d, i + 2, n] + f_ref[d, i + 3, n]) + (
                    (up_ref[d, i + 1, n] - down_ref[d, i + 3, n]) - ahead
                )

            combine(d, h + (15 if d else 21), h, wave, linear)
            if d:
                for k in range(3):
                    turn_back(jnp.minimum(3 * h + k, NVAR - 1))
            return 0

        lax.fori_loop(first, last, step, 0)

    for side, first in ((0, ny - 3), (1, 0)):
        for k in range(3):
            for r in range(NVAR):
                sy_ref[side, k, r] = turned(r, first + k)

    def x_state(x, best):
        u = [own(r, x) for r in range(NVAR)]
        inverse, vel, temp, pressure, gamma, sound = thermo(u, table_ref)
        for k, value in enumerate([inverse, *vel, temp, pressure, gamma, sound]):
            cache_ref[x, k] = value
        return tuple(jnp.maximum(b, jnp.abs(v) + sound) for b, v in zip(best, vel))

    zero = jnp.zeros(tile, jnp.float32)
    best = lax.fori_loop(0, 8, x_state, (zero, zero, zero), unroll=2)
    best = [jnp.max(b, axis=(0, 1), keepdims=True) for b in best]
    column = lax.broadcasted_iota(jnp.int32, (1, lanes), 1)
    mine_ref[...] = jnp.where(column == 0, best[0], jnp.where(column == 1, best[1], best[2]))
    def x_cells(x, _):
        u = [own(r, x) for r in range(NVAR)]
        state = [cache_ref[x, k] for k in range(8)]
        cells(0, x + 3, u, (state[0], state[1:4], *state[4:]))
        return 0

    for r in range(NVAR):
        z_ref[pl.ds(r * block, block), :] = flip(x_ref[pl.ds(r * block, block), :])
    lax.fori_loop(0, 8, x_cells, 0)
    pl.semaphore_wait(barrier, len(others))

    for n, (ox, oy) in enumerate(others):
        copy = pltpu.make_async_remote_copy(
            src_ref=mine_ref,
            dst_ref=slots_ref.at[n],
            send_sem=small_send,
            recv_sem=small_recv,
            device_id=there(ox, oy),
            device_id_type=MESH,
        )
        copy.start()
    own_cells(1, turned)
    own_cells(2, upright)

    lane = lax.broadcasted_iota(jnp.int32, tile, 1)
    row = lax.broadcasted_iota(jnp.int32, tile, 0)
    walls = kind_ref[0] == 1, kind_ref[1] == 1
    outside = (row == 0) & (lane < block), (row == 7) & (lane >= block)
    wrap = row == 0, row == 7

    def beyond(side, r, k):
        inner = upright(r, (7 - k) if side else (2 - k))
        edge = upright(r, 7 if side else 0)
        ghost = jnp.where(walls[side], -inner if r == NS + 2 else inner, edge)
        if side:
            along = pltpu.roll(upright(r, k), 7, 0)
        else:
            along = pltpu.roll(upright(r, 5 + k), 1, 0)
        across = pltpu.roll(along, block, 1)
        return jnp.where(outside[side], ghost, jnp.where(wrap[side], across, along))

    halos = []
    for n, (origin, target, device) in enumerate(
        (
            (planes_ref.at[:, pl.ds(nx - 3, 3)], hx_ref.at[0], there(1, 0)),
            (planes_ref.at[:, pl.ds(0, 3)], hx_ref.at[1], there(size_x - 1, 0)),
            (sy_ref.at[0], hy_ref.at[0], there(0, 1)),
            (sy_ref.at[1], hy_ref.at[1], there(0, size_y - 1)),
        )
    ):
        copy = pltpu.make_async_remote_copy(
            src_ref=origin,
            dst_ref=target,
            send_sem=big_send.at[n],
            recv_sem=big_recv.at[n],
            device_id=device,
            device_id_type=MESH,
        )
        copy.start()
        halos.append(copy)

    for side in range(2):
        halo_cells(2, side, beyond)
    differences(0, 3, 10)
    differences(1, 3, 10)
    differences(2, 0, 13)
    project(2, 0, 9, 0)
    project(1, 3, 6, 9)
    project(0, 3, 6, 12)

    for sem in (small_recv, small_send):
        pltpu.make_async_copy(slots_ref, slots_ref, sem).wait()
    value = jnp.maximum(mine_ref[...], jnp.max(slots_ref[...], axis=0))
    alphas = [
        jnp.broadcast_to(
            jnp.max(jnp.where(column == d, value, 0.0), axis=1, keepdims=True), tile
        )
        for d in range(3)
    ]
    scale = (-COURANT / 6.0) / (alphas[0] + alphas[1] + alphas[2])

    advance(2, 0, 9)
    advance(1, 9, 12)
    advance(0, 12, 15)
    for copy in halos[2:]:
        copy.wait()
    for r in range(NVAR):
        for i in range(8):
            back_ref[pl.ds(r * block + i, 8, stride=8), :] = rate(2, i, r)
    for side in range(2):
        halo_cells(1, side, lambda side, r, k: hy_ref[side, k, r])
    split_inner(1)
    split_outer(1, 0)
    split_outer(1, 10)
    lay(1, 0, 6)
    close(1, 0, 6)
    split_inner(0)
    for side, copy in enumerate(halos[:2]):
        copy.wait()
        for r in range(NVAR):
            if r % 2 == side:
                gather_y(r)
        halo_cells(0, side, lambda side, r, k: hx_ref[side, r, k])
        split_outer(0, 10 * side)
        lay(0, 3 * side, 3 * side + 3)
        close(0, 3 * side, 3 * side + 3)
    for r in range(NVAR):
        for i in range(8):
            rows = pl.ds(r * block + i * 8, 8)
            out_ref[rows, :] = scale * (rate(0, i, r) + acc_ref[rows, :] + z_ref[rows, :])


def shards(preserved_vector, nasa_table, gas_constant, species_index, face_kind):
    _, nx, ny, lanes = preserved_vector.shape
    size_x, size_y = lax.axis_size("gx"), lax.axis_size("gy")
    others = size_x * size_y - 1
    flat = preserved_vector.reshape(NVAR * nx * ny, lanes)
    hbm = pl.BlockSpec(memory_space=pltpu.HBM)
    dma = pltpu.SemaphoreType.DMA

    def buffer(*shape):
        return pltpu.VMEM(shape + (8, lanes), jnp.float32)

    out = pl.pallas_call(
        functools.partial(fused, size_x, size_y),
        out_shape=pltpu.VMEM(flat.shape, jnp.float32),
        in_specs=[hbm] * 6,
        out_specs=pl.BlockSpec(memory_space=pltpu.VMEM),
        scratch_shapes=[
            pltpu.SMEM(nasa_table.T.shape, jnp.float32),
            pltpu.SMEM(gas_constant.shape, jnp.float32),
            pltpu.SMEM(species_index.shape, jnp.int32),
            pltpu.SMEM((2,), jnp.int32),
            *[pltpu.VMEM(flat.shape, jnp.float32) for _ in range(4)],
            buffer(2, NVAR, 3),
            buffer(2, 3, NVAR),
            buffer(2, 3, NVAR),
            pltpu.VMEM((1, lanes), jnp.float32),
            pltpu.VMEM((others, 1, lanes), jnp.float32),
            buffer(TABLE),
            buffer(8, 8),
            buffer(3, 10, PRIMS),
            buffer(3, 14, NVAR + 1),
            buffer(3, 14, NVAR + 1),
            buffer(3, 13, NVAR + 1),
            buffer(3, 13, NVAR + 1),
            buffer(15, NVAR * ROW),
            buffer(15, COEFS),
            buffer(3 * FACES, NVAR),
            buffer(2, 13, NVAR + 1),
            buffer(2, 13, NVAR + 1),
            dma(()),
            dma((4,)),
            dma(()),
            dma(()),
            dma((4,)),
            dma((4,)),
        ],
        compiler_params=pltpu.CompilerParams(
            collective_id=0, has_side_effects=True, vmem_limit_bytes=60 * 1000 * 1000
        ),
        name="increment",
    )(
        nasa_table.T, gas_constant, species_index, face_kind.reshape(2), flat,
        preserved_vector,
    )
    return out.reshape(preserved_vector.shape)


def solution(mesh):
    return jax.shard_map(
        shards,
        mesh=mesh,
        in_specs=(P(None, "gx", "gy", None), P(), P(), P(), P("gx", "gy", None)),
        out_specs=P(None, "gx", "gy", None),
        check_vma=False,
    )
```

```python
import functools

import jax
import jax.numpy as jnp
from jax import lax
from jax.experimental import pallas as pl
from jax.experimental.pallas import tpu as pltpu
from jax.sharding import PartitionSpec as P

NS = 9
NVAR = 14
EPSILON = 1e-06
COURANT = 0.8
TOTAL = NVAR
PRIMS = 24
VEL, PASSIVE, GAMMA, SOUND, SLOPES = 9, 12, 13, 14, 15
TABLE = 7 * NS
ORDER = ((0, 1, 2), (1, 0, 2), (2, 0, 1))
PARTS = 7
ROW = 2 * PARTS + 2
STEEP, ENTHALPY, SQUARE = 14, 23, 24
COEFS = 25
FACES = 9
MESH = pl.DeviceIdType.MESH


def fill_table(nasa_ref, gas_ref, index_ref, table_ref):
    for i in range(NS):
        row = index_ref[i]
        gas = gas_ref[row]
        values = [
            gas,
            gas * nasa_ref[5, row],
            gas * (nasa_ref[0, row] - 1.0),
            gas * nasa_ref[1, row] * (1.0 / 2.0),
            gas * nasa_ref[2, row] * (1.0 / 3.0),
            gas * nasa_ref[3, row] * (1.0 / 4.0),
            gas * nasa_ref[4, row] * (1.0 / 5.0),
        ]
        for n, value in enumerate(values):
            table_ref[n * NS + i] = jnp.full(table_ref.shape[1:], value, jnp.float32)


def tree(terms):
    terms = list(terms)
    while len(terms) > 1:
        terms = [a + b for a, b in zip(terms[::2], terms[1::2])] + (
            [terms[-1]] if len(terms) % 2 else []
        )
    return terms[0]


def thermo(u, table_ref):
    rho = tree(u[:NS])
    inverse = 1.0 / rho
    vel = [m * inverse for m in u[NS : NS + 3]]
    inner = u[NS + 3] - 0.5 * tree([v * m for v, m in zip(vel, u[NS : NS + 3])])
    mix = [tree([u[i] * table_ref[n * NS + i] for i in range(NS)]) for n in range(7)]
    gas, m6, m1, m2, m3, m4, m5 = mix
    c2, c3, c4, c5 = 2.0 * m2, 3.0 * m3, 4.0 * m4, 5.0 * m5
    temp = 1.0 - (tree([m6, m1, m2, m3, m4, m5]) - inner) / tree([m1, c2, c3, c4, c5])

    def heat(t):
        return m1 + t * (c2 + t * (c3 + t * (c4 + t * c5)))

    energy = m6 + temp * (m1 + temp * (m2 + temp * (m3 + temp * (m4 + temp * m5))))
    temp = temp - (energy - inner) / heat(temp)
    pressure = temp * gas
    gamma = gas / heat(temp)
    sound = jnp.sqrt((1.0 + gamma) * pressure * inverse)
    return inverse, vel, temp, pressure, gamma, sound


def half_slopes(temp, gamma, vel, table_ref):
    warm, lean = 0.5 * temp, 0.5 * gamma
    kinetic = (0.5 * lean) * tree([v * v for v in vel])
    result = []
    for i in range(NS):
        k = [table_ref[n * NS + i] for n in range(7)]
        e = k[1] + temp * (k[2] + temp * (k[3] + temp * (k[4] + temp * (k[5] + temp * k[6]))))
        result.append(k[0] * warm - lean * e + kinetic)
    return result


def reciprocal(x):
    return pl.reciprocal(x, approx=True)


def correction(d1, d2, e0, e1, e2):
    h1, h2 = 0.75 * d1, 0.75 * d2
    near, far = h1 * d1 + 0.75 * EPSILON, h2 * d2 + 0.75 * EPSILON
    r0 = reciprocal(e0 * (e0 + h1) + near)
    r1 = reciprocal(e1 * (e1 + h1) + near)
    r2 = reciprocal(e2 * (e2 - h2) + far)
    a = r0 * r0 * (1.0 / 3.0)
    b = r1 * r1
    c = r2 * r2
    g0, g2 = e0 - e1, e1 - e2
    return (a * (g0 + g0) + c * g2) * reciprocal(a + c + (b + b))


def fused(
    size_x, size_y,
    nasa_hbm, gas_hbm, index_hbm, kind_hbm, flat_ref, planes_ref, out_ref,
    nasa_ref, gas_ref, index_ref, kind_ref,
    x_ref, z_ref, acc_ref, back_ref, hx_ref, sy_ref, hy_ref, mine_ref, slots_ref,
    table_ref, cache_ref, prim_ref, f_ref, u_ref, df_ref, du_ref,
    part_ref, coef_ref, flux_ref, up_ref, down_ref,
    load_sem, param_sem, small_send, small_recv, big_send, big_recv,
):
    load = pltpu.make_async_copy(flat_ref, x_ref, load_sem)
    load.start()
    params = [
        pltpu.make_async_copy(origin, target, param_sem.at[n])
        for n, (origin, target) in enumerate(
            (
                (nasa_hbm, nasa_ref),
                (gas_hbm, gas_ref),
                (index_hbm, index_ref),
                (kind_hbm, kind_ref),
            )
        )
    ]
    for copy in params:
        copy.start()
    gx, gy = lax.axis_index("gx"), lax.axis_index("gy")
    nx, ny = planes_ref.shape[1], planes_ref.shape[2]
    lanes = x_ref.shape[1]
    tile = (8, lanes)
    block = nx * ny

    def there(ox, oy):
        return (lax.rem(gx + ox, size_x), lax.rem(gy + oy, size_y))

    others = [(ox, oy) for ox in range(size_x) for oy in range(size_y) if ox or oy]
    barrier = pltpu.get_barrier_semaphore()
    for ox, oy in others:
        pl.semaphore_signal(barrier, inc=1, device_id=there(ox, oy), device_id_type=MESH)
    for copy in params:
        copy.wait()
    fill_table(nasa_ref, gas_ref, index_ref, table_ref)
    load.wait()

    def own(r, x):
        return x_ref[pl.ds(pl.multiple_of(r * block + x * 8, 8), 8), :]

    def turned(r, y):
        return x_ref[pl.ds(r * block + y, 8, stride=8), :]

    def upright(r, t):
        return z_ref[pl.ds(r * block + t, 8, stride=8), :]

    def flow(d, p, u, vel, pressure):
        order = ORDER[d]
        speed = vel[order[0]]
        half, push = 0.5 * speed, 0.5 * pressure
        rows = list(range(NS)) + [NS + n for n in order] + [NS + 3, NS + 4]
        for k, r in enumerate(rows):
            value = u[r] * half
            if k == NS:
                value = value + push
            if k == NS + 3:
                value = value + push * speed
            f_ref[d, p, k] = value
            u_ref[d, p, k] = 0.5 * u[r]
        rho = tree(u[:NS])
        f_ref[d, p, TOTAL] = rho * half
        u_ref[d, p, TOTAL] = 0.5 * rho

    def cells(d, p, u, state):
        inverse, vel, temp, pressure, gamma, sound = state
        flow(d, p, u, vel, pressure)
        q = p - 2
        share = 0.5 * inverse
        for k in range(NS):
            prim_ref[d, q, k] = u[k] * share
        for k in range(3):
            prim_ref[d, q, VEL + k] = 0.5 * vel[ORDER[d][k]]
        prim_ref[d, q, PASSIVE] = u[NS + 4] * share
        prim_ref[d, q, GAMMA] = 0.5 * gamma
        prim_ref[d, q, SOUND] = 0.5 * sound
        for k, value in enumerate(half_slopes(temp, gamma, vel, table_ref)):
            prim_ref[d, q, SLOPES + k] = value

    def own_cells(d, read):
        def step(n, _):
            u = [read(r, n) for r in range(NVAR)]
            cells(d, n + 3, u, thermo(u, table_ref))
            return 0

        lax.fori_loop(0, 8, step, 0, unroll=2)

    def halo_cells(d, side, read):
        for k in range(3):
            p = k + 11 * side
            u = [read(side, r, k) for r in range(NVAR)]
            state = thermo(u, table_ref)
            if p in (2, 11):
                cells(d, p, u, state)
            else:
                flow(d, p, u, state[1], state[3])

    def differences(d, first, last):
        def step(p, _):
            for k in range(NVAR + 1):
                df_ref[d, p, k] = f_ref[d, p + 1, k] - f_ref[d, p, k]
                du_ref[d, p, k] = u_ref[d, p + 1, k] - u_ref[d, p, k]
            return 0

        lax.fori_loop(first, last, step, 0)

    def split_inner(d):
        def step(p, _):
            for k in range(NVAR + 1):
                push = alphas[d] * du_ref[d, p, k]
                up_ref[d, p, k] = df_ref[d, p, k] + push
                down_ref[d, p, k] = df_ref[d, p, k] - push
            return 0

        lax.fori_loop(3, 10, step, 0)

    def split_outer(d, first):
        def step(p, _):
            for k in range(NVAR + 1):
                step_f = f_ref[d, p + 1, k] - f_ref[d, p, k]
                push = alphas[d] * (u_ref[d, p + 1, k] - u_ref[d, p, k])
                up_ref[d, p, k] = step_f + push
                down_ref[d, p, k] = step_f - push
            return 0

        lax.fori_loop(first, first + 3, step, 0)

    def means(d, i):
        def mean(q):
            return prim_ref[d, i, q] + prim_ref[d, i + 1, q]

        y = [mean(k) for k in range(NS)]
        vel = [mean(VEL + k) for k in range(3)]
        phi = [mean(SLOPES + k) for k in range(NS)]
        return y, vel, phi, mean(PASSIVE), mean(GAMMA), mean(SOUND)

    def keep_means(d, i, g):
        y, vel, phi, z, gamma, sound = means(d, i)
        inv = 1.0 / sound
        steep = 1.0 / gamma
        for k in range(NS):
            coef_ref[g, k] = y[k]
            coef_ref[g, STEEP + k] = phi[k] * steep
        for k in range(3):
            coef_ref[g, VEL + k] = vel[k]
        coef_ref[g, PASSIVE] = z
        coef_ref[g, GAMMA] = sound
        coef_ref[g, ENTHALPY] = (sound * sound - tree([a * b for a, b in zip(y, phi)])) * steep
        coef_ref[g, SQUARE] = tree([v * v for v in vel])
        return y, vel, phi, z, gamma, inv * inv, 0.5 * inv

    def waves_of(get, vel, phi, gamma, inv2, half_inv):
        s = get(TOTAL)
        m = [get(NS + n) for n in range(3)]
        dp = tree([phi[n] * get(n) for n in range(NS)]) + gamma * (
            get(NS + 3) - tree([vel[n] * m[n] for n in range(3)])
        )
        scaled = dp * inv2
        jump = (m[0] - vel[0] * s) * half_inv
        middle = 0.5 * scaled
        return scaled, middle - jump, m[1] - vel[1] * s, m[2] - vel[2] * s, middle + jump

    def project(d, first, last, start):
        def step(i, _):
            g = i + (start - first)
            y, vel, phi, z, gamma, inv2, half_inv = keep_means(d, i, g)
            for half, ref in enumerate((df_ref, du_ref)):

                def keep(n, d5):
                    at = n * ROW + half * PARTS
                    for j in range(3):
                        part_ref[g, at + j] = d5[j + 1]
                    for j in range(4):
                        part_ref[g, at + 3 + j] = d5[j + 1] - d5[j]

                waves = [
                    waves_of(lambda n: ref[d, i + k, n], vel, phi, gamma, inv2, half_inv)
                    for k in range(5)
                ]
                for n in range(4):
                    keep(NS + n, [w[n + 1] for w in waves])
                for n, share in enumerate(y):
                    keep(n, [ref[d, i + k, n] - share * waves[k][0] for k in range(5)])
                keep(NS + 4, [ref[d, i + k, NS + 4] - z * waves[k][0] for k in range(5)])
            for n in range(NVAR):
                part_ref[g, n * ROW + 2 * PARTS] = 6.0 * (
                    f_ref[d, i + 2, n] + f_ref[d, i + 3, n]
                ) + (df_ref[d, i + 1, n] - df_ref[d, i + 3, n])
                centre = du_ref[d, i + 2, n]
                part_ref[g, n * ROW + 2 * PARTS + 1] = (du_ref[d, i + 1, n] - centre) + (
                    du_ref[d, i + 3, n] - centre
                )
            return 0

        lax.fori_loop(first, last, step, 0)

    def combine(d, g, c, wave, linear):
        slower, faster = wave(NS), wave(NS + 3)
        shears = [wave(NS + 1), wave(NS + 2)]
        acoustic = slower + faster
        total, weighted = None, None
        for n in range(NS):
            amp = wave(n)
            flux_ref[g, n] = linear(n) + coef_ref[c, n] * acoustic + amp
            steep = coef_ref[c, STEEP + n] * amp
            total = amp if n == 0 else total + amp
            weighted = steep if n == 0 else weighted + steep
        amp = wave(NS + 4)
        flux_ref[g, NS + 4] = linear(NS + 4) + coef_ref[c, PASSIVE] * acoustic + amp
        mass = acoustic + total
        swing = coef_ref[c, GAMMA] * (faster - slower)
        vel = [coef_ref[c, VEL + n] for n in range(3)]
        moved = [swing] + shears
        for n, r in enumerate(ORDER[d]):
            flux_ref[g, NS + r] = linear(NS + n) + vel[n] * mass + moved[n]
        flux_ref[g, NS + 3] = (
            linear(NS + 3)
            + coef_ref[c, SQUARE] * mass
            + (coef_ref[c, ENTHALPY] * acoustic - weighted)
            + tree([v * m for v, m in zip(vel, moved)])
        )

    def advance(d, first, last):
        def step(g, _):
            alpha = alphas[d]

            def wave(n):
                f = [part_ref[g, n * ROW + j] for j in range(PARTS)]
                t = [alpha * part_ref[g, n * ROW + PARTS + j] for j in range(PARTS)]
                rising = correction(f[0] + t[0], f[1] + t[1], f[3] + t[3], f[4] + t[4], f[5] + t[5])
                falling = correction(f[2] - t[2], f[1] - t[1], t[6] - f[6], t[5] - f[5], t[4] - f[4])
                return rising - falling

            def linear(n):
                at = n * ROW + 2 * PARTS
                return part_ref[g, at] + alpha * part_ref[g, at + 1]

            combine(d, g, g, wave, linear)
            return 0

        lax.fori_loop(first, last, step, 0, unroll=3)

    side_by_side = lax.broadcasted_iota(jnp.int32, (block, lanes), 1) < block

    def flip(a):
        b = jnp.concatenate([a, a], axis=0).T
        return jnp.where(side_by_side, b[:block], b[block:])

    def turn_back(r):
        rows = pl.ds(pl.multiple_of(r * block, block), block)
        z_ref[rows, :] = flip(back_ref[rows, :])

    def slot(d, i):
        if d == 2:
            return i
        if 3 <= i < 6:
            return (9 if d else 12) + i - 3
        return (15 if d else 21) + (i if i < 3 else i - 3)

    def rate(d, i, r):
        return flux_ref[slot(d, i + 1), r] - flux_ref[slot(d, i), r]

    def gather_y(r):
        for i in range(8):
            acc_ref[pl.ds(r * block + i, 8, stride=8), :] = rate(1, i, r)

    def outer_face(h):
        return jnp.where(h < 3, h, h + 3)

    def lay(d, first, last):
        def step(h, _):
            i = outer_face(h)
            y, vel, phi, z, gamma, inv2, half_inv = keep_means(d, i, h)
            for side, get in enumerate(
                (
                    lambda n, k: up_ref[d, i + k, n],
                    lambda n, k: down_ref[d, i + 4 - k, n],
                )
            ):
                for k in range(4):
                    at = 4 * side + k
                    waves = waves_of(lambda n: get(n, k), vel, phi, gamma, inv2, half_inv)
                    for n in range(4):
                        part_ref[h, (NS + n) * 8 + at] = waves[n + 1]
                    for n in range(NS):
                        part_ref[h, n * 8 + at] = get(n, k) - y[n] * waves[0]
                    part_ref[h, (NS + 4) * 8 + at] = get(NS + 4, k) - z * waves[0]
            return 0

        lax.fori_loop(first, last, step, 0, unroll=3)

    def close(d, first, last):
        def step(h, _):
            i = outer_face(h)

            def wave(n):
                pair = []
                for side in range(2):
                    v = [part_ref[h, n * 8 + side * 4 + k] for k in range(4)]
                    pair.append(correction(v[1], v[2], v[1] - v[0], v[2] - v[1], v[3] - v[2]))
                return pair[0] - pair[1]

            def linear(n):
                ahead = up_ref[d, i + 2, n] - down_ref[d, i + 2, n]
                return 6.0 * (f_ref[d, i + 2, n] + f_ref[d, i + 3, n]) + (
                    (up_ref[d, i + 1, n] - down_ref[d, i + 3, n]) - ahead
                )

            combine(d, h + (15 if d else 21), h, wave, linear)
            if d:
                for k in range(3):
                    turn_back(jnp.minimum(3 * h + k, NVAR - 1))
            return 0

        lax.fori_loop(first, last, step, 0, unroll=3)

    for side, first in ((0, ny - 3), (1, 0)):
        for k in range(3):
            for r in range(NVAR):
                sy_ref[side, k, r] = turned(r, first + k)

    def x_state(x, best):
        u = [own(r, x) for r in range(NVAR)]
        inverse, vel, temp, pressure, gamma, sound = thermo(u, table_ref)
        for k, value in enumerate([inverse, *vel, temp, pressure, gamma, sound]):
            cache_ref[x, k] = value
        return tuple(jnp.maximum(b, jnp.abs(v) + sound) for b, v in zip(best, vel))

    zero = jnp.zeros(tile, jnp.float32)
    best = lax.fori_loop(0, 8, x_state, (zero, zero, zero), unroll=2)
    best = [jnp.max(b, axis=(0, 1), keepdims=True) for b in best]
    column = lax.broadcasted_iota(jnp.int32, (1, lanes), 1)
    mine_ref[...] = jnp.where(column == 0, best[0], jnp.where(column == 1, best[1], best[2]))
    def x_cells(x, _):
        u = [own(r, x) for r in range(NVAR)]
        state = [cache_ref[x, k] for k in range(8)]
        cells(0, x + 3, u, (state[0], state[1:4], *state[4:]))
        return 0

    for r in range(NVAR):
        z_ref[pl.ds(r * block, block), :] = flip(x_ref[pl.ds(r * block, block), :])
    lax.fori_loop(0, 8, x_cells, 0)
    pl.semaphore_wait(barrier, len(others))

    for n, (ox, oy) in enumerate(others):
        copy = pltpu.make_async_remote_copy(
            src_ref=mine_ref,
            dst_ref=slots_ref.at[n],
            send_sem=small_send,
            recv_sem=small_recv,
            device_id=there(ox, oy),
            device_id_type=MESH,
        )
        copy.start()
    own_cells(1, turned)
    own_cells(2, upright)

    lane = lax.broadcasted_iota(jnp.int32, tile, 1)
    row = lax.broadcasted_iota(jnp.int32, tile, 0)
    walls = kind_ref[0] == 1, kind_ref[1] == 1
    outside = (row == 0) & (lane < block), (row == 7) & (lane >= block)
    wrap = row == 0, row == 7

    def beyond(side, r, k):
        inner = upright(r, (7 - k) if side else (2 - k))
        edge = upright(r, 7 if side else 0)
        ghost = jnp.where(walls[side], -inner if r == NS + 2 else inner, edge)
        if side:
            along = pltpu.roll(upright(r, k), 7, 0)
        else:
            along = pltpu.roll(upright(r, 5 + k), 1, 0)
        across = pltpu.roll(along, block, 1)
        return jnp.where(outside[side], ghost, jnp.where(wrap[side], across, along))

    halos = []
    for n, (origin, target, device) in enumerate(
        (
            (planes_ref.at[:, pl.ds(nx - 3, 3)], hx_ref.at[0], there(1, 0)),
            (planes_ref.at[:, pl.ds(0, 3)], hx_ref.at[1], there(size_x - 1, 0)),
            (sy_ref.at[0], hy_ref.at[0], there(0, 1)),
            (sy_ref.at[1], hy_ref.at[1], there(0, size_y - 1)),
        )
    ):
        copy = pltpu.make_async_remote_copy(
            src_ref=origin,
            dst_ref=target,
            send_sem=big_send.at[n],
            recv_sem=big_recv.at[n],
            device_id=device,
            device_id_type=MESH,
        )
        copy.start()
        halos.append(copy)

    for side in range(2):
        halo_cells(2, side, beyond)
    differences(0, 3, 10)
    differences(1, 3, 10)
    differences(2, 0, 13)
    project(2, 0, 9, 0)
    project(1, 3, 6, 9)
    project(0, 3, 6, 12)

    for sem in (small_recv, small_send):
        pltpu.make_async_copy(slots_ref, slots_ref, sem).wait()
    value = jnp.maximum(mine_ref[...], jnp.max(slots_ref[...], axis=0))
    alphas = [
        jnp.broadcast_to(
            jnp.max(jnp.where(column == d, value, 0.0), axis=1, keepdims=True), tile
        )
        for d in range(3)
    ]
    scale = (-COURANT / 6.0) / (alphas[0] + alphas[1] + alphas[2])

    advance(2, 0, 9)
    advance(1, 9, 12)
    advance(0, 12, 15)
    for copy in halos[2:]:
        copy.wait()
    for r in range(NVAR):
        for i in range(8):
            back_ref[pl.ds(r * block + i, 8, stride=8), :] = rate(2, i, r)
    for side in range(2):
        halo_cells(1, side, lambda side, r, k: hy_ref[side, k, r])
    split_inner(1)
    split_outer(1, 0)
    split_outer(1, 10)
    lay(1, 0, 6)
    close(1, 0, 6)
    split_inner(0)
    for side, copy in enumerate(halos[:2]):
        copy.wait()
        for r in range(NVAR):
            if r % 2 == side:
                gather_y(r)
        halo_cells(0, side, lambda side, r, k: hx_ref[side, r, k])
        split_outer(0, 10 * side)
        lay(0, 3 * side, 3 * side + 3)
        close(0, 3 * side, 3 * side + 3)
    for r in range(NVAR):
        for i in range(8):
            rows = pl.ds(r * block + i * 8, 8)
            out_ref[rows, :] = scale * (rate(0, i, r) + acc_ref[rows, :] + z_ref[rows, :])


def shards(preserved_vector, nasa_table, gas_constant, species_index, face_kind):
    _, nx, ny, lanes = preserved_vector.shape
    size_x, size_y = lax.axis_size("gx"), lax.axis_size("gy")
    others = size_x * size_y - 1
    flat = preserved_vector.reshape(NVAR * nx * ny, lanes)
    hbm = pl.BlockSpec(memory_space=pltpu.HBM)
    dma = pltpu.SemaphoreType.DMA

    def buffer(*shape):
        return pltpu.VMEM(shape + (8, lanes), jnp.float32)

    out = pl.pallas_call(
        functools.partial(fused, size_x, size_y),
        out_shape=pltpu.VMEM(flat.shape, jnp.float32),
        in_specs=[hbm] * 6,
        out_specs=pl.BlockSpec(memory_space=pltpu.VMEM),
        scratch_shapes=[
            pltpu.SMEM(nasa_table.T.shape, jnp.float32),
            pltpu.SMEM(gas_constant.shape, jnp.float32),
            pltpu.SMEM(species_index.shape, jnp.int32),
            pltpu.SMEM((2,), jnp.int32),
            *[pltpu.VMEM(flat.shape, jnp.float32) for _ in range(4)],
            buffer(2, NVAR, 3),
            buffer(2, 3, NVAR),
            buffer(2, 3, NVAR),
            pltpu.VMEM((1, lanes), jnp.float32),
            pltpu.VMEM((others, 1, lanes), jnp.float32),
            buffer(TABLE),
            buffer(8, 8),
            buffer(3, 10, PRIMS),
            buffer(3, 14, NVAR + 1),
            buffer(3, 14, NVAR + 1),
            buffer(3, 13, NVAR + 1),
            buffer(3, 13, NVAR + 1),
            buffer(15, NVAR * ROW),
            buffer(15, COEFS),
            buffer(3 * FACES, NVAR),
            buffer(2, 13, NVAR + 1),
            buffer(2, 13, NVAR + 1),
            dma(()),
            dma((4,)),
            dma(()),
            dma(()),
            dma((4,)),
            dma((4,)),
        ],
        compiler_params=pltpu.CompilerParams(
            collective_id=0, has_side_effects=True, vmem_limit_bytes=60 * 1000 * 1000
        ),
        name="increment",
    )(
        nasa_table.T, gas_constant, species_index, face_kind.reshape(2), flat,
        preserved_vector,
    )
    return out.reshape(preserved_vector.shape)


def solution(mesh):
    return jax.shard_map(
        shards,
        mesh=mesh,
        in_specs=(P(None, "gx", "gy", None), P(), P(), P(), P("gx", "gy", None)),
        out_specs=P(None, "gx", "gy", None),
        check_vma=False,
    )
```
